128 devices in a mesh: tm: 8 (over y, x_lo), inp: 16 (over z, x_hi, core).
Axes of the slice: x: 4 (x_hi: 2, x_lo: 2; x = x_hi * 2 + x_lo), y: 4, z: 4, core: 2. Of those that a mesh axis runs over, the one named last changes fastest.
Arguments:
- voltages: bfloat16 [1024, 1048576], P('inp', 'tm'), may hold values from -6 to 6
- coefficients: float32 [16, 8192], replicated, may hold values from -1.5 to 1.5
Outputs:
- visibilities: float32 [2, 128, 1024, 1024], P(None, ('tm', 'inp'))
The draws below stay inside these ranges and needn't reach their ends.
All inputs are finite; a program needn't handle non-finite values.
Results may differ from the reference program's by a relative error of at most 0.0003.
Values may be sent and summed in bfloat16 or wider, within the bound.
No kernel may reach another device: no remote copies, remote signals or barrier semaphores. Data moves between devices by JAX's collectives and lax.ppermute only.
A program may use at most 192 MiB of HBM per device.

```python
import math
import jax
import jax.numpy as jnp
from jax import lax

NFFT = 8192
TAPS = 16
INPUTS = 1024
CH = 128
CH0 = 1024
SPECTRA = 128
SAMPLES = 1048576


def block_levels(key, shape, shards, smallest, largest):
    loudness, own = 1.0, jax.random.fold_in(key, 6)
    for position, parts in shards:
        steps = jnp.exp(jax.random.uniform(jax.random.fold_in(own, position), (parts,), jnp.float32, smallest / len(shards), largest / len(shards)))
        loudness = loudness * jnp.repeat(steps, shape[position] // parts).reshape([-1 if axis == position else 1 for axis in range(len(shape))])
    return loudness


def gaussian(rng, extent, width, bound, pieces=(), kind=jnp.bfloat16):
    level = block_levels(rng, extent, pieces, -0.22, 0.18) if pieces else 1.0
    array = jax.random.normal(rng, extent, jnp.float32) * width * level
    return jnp.minimum(jnp.maximum(array, -bound), bound).astype(kind)


def setup_inputs(seed: int = 0) -> dict:
    seeds = jax.random.split(jax.random.key(seed), 3)
    return {
        "voltages": gaussian(seeds[0], (INPUTS, SAMPLES), 1.0, 6.0, ((0, 16), (1, 8))),
        "coefficients": gaussian(seeds[1], (TAPS, NFFT), 0.25, 1.5, (), jnp.float32),
    }


def channelize(row, coefficients):
    signal = row.astype(jnp.float32)
    padded = jnp.concatenate([jnp.zeros((TAPS - 1, NFFT), jnp.float32), signal], axis=0)
    filtered = jnp.zeros((SPECTRA, NFFT), jnp.float32)
    for tap in range(TAPS):
        filtered = filtered + coefficients[tap] * padded[TAPS - 1 - tap:TAPS - 1 - tap + SPECTRA]
    spectrum = jnp.fft.rfft(filtered, axis=-1)[:, CH0:CH0 + CH] * (NFFT ** -0.5)
    return jnp.stack([jnp.real(spectrum), jnp.imag(spectrum)]).astype(filtered.dtype)


def correlate(pair):
    real_part, imag_part = pair[0], pair[1]
    vis_real = jnp.dot(real_part.T, real_part, precision=lax.Precision.HIGHEST) + jnp.dot(imag_part.T, imag_part, precision=lax.Precision.HIGHEST)
    cross = jnp.dot(imag_part.T, real_part, precision=lax.Precision.HIGHEST)
    vis_imag = cross - cross.T
    return jnp.stack([vis_real, vis_imag]) / SPECTRA


def reference(voltages, coefficients):
    frames = voltages.reshape(INPUTS, SPECTRA, NFFT)
    group = math.gcd(INPUTS, 16)
    grouped = frames.reshape(INPUTS // group, group, SPECTRA, NFFT)
    spectra = lax.map(lambda block: jax.vmap(lambda row: channelize(row, coefficients))(block), grouped)
    spectra = spectra.reshape(INPUTS, 2, SPECTRA, CH).transpose(3, 1, 2, 0)
    result = lax.map(correlate, spectra)
    return result.transpose(1, 0, 2, 3)
```

```python
import functools

import jax
import jax.numpy as jnp
import numpy as np
from jax import lax
from jax.experimental import pallas as pl
from jax.experimental.pallas import tpu as pltpu
from jax.sharding import PartitionSpec as P

NFFT = 8192
TAPS = 16
CH = 128
CH0 = 1024
LANES = 128
CHUNK = 256
ROWS = 16
F32 = jnp.float32
BF16 = jnp.bfloat16


def twiddles():
    channel = CH0 + np.arange(CH)
    small = 2.0 * np.pi / NFFT * (np.arange(CHUNK)[:, None] * channel[None, :] % NFFT)
    base = 2.0 * np.pi / NFFT * (np.arange(NFFT // CHUNK)[:, None] * CHUNK * channel[None, :] % NFFT)
    small = np.stack([np.cos(small), -np.sin(small)]) * NFFT ** (-0.5)
    base = np.stack([np.cos(base), -np.sin(base)], axis=1)
    return jnp.asarray(small, F32), jnp.asarray(base, F32)


def split(value):
    high = value.astype(BF16)
    return high, (value - high.astype(F32)).astype(BF16)


def terms(carried, frames):
    if carried:
        return [[(t, frames + s - t) for t in range(s + 1, TAPS)] for s in range(TAPS - 1)]
    return [[(t, s - t) for t in range(min(s, TAPS - 1) + 1)] for s in range(frames)]


def channelize(carried, frames, inputs, *refs):
    x_refs, (h_ref, small_ref, base_ref, out_ref) = refs[:frames], refs[frames : frames + 4]
    slots, acc_ref = (refs[frames + 4 : frames + 8], refs[frames + 8 : frames + 12]), refs[frames + 12]
    plan = terms(carried, frames)
    step = pl.program_id(0)

    @pl.when(step == 0)
    def _():
        acc_ref[...] = jnp.zeros_like(acc_ref)
        for ref in slots[1]:
            ref[...] = jnp.zeros_like(ref)

    def fill(part):
        high_ref, low_ref, table_high_ref, table_low_ref = slots[part]
        base = base_ref[2 * step + part]
        real, imag = small_ref[0], small_ref[1]
        turn_real, turn_imag = base[0:1], base[1:2]
        table = (real * turn_real - imag * turn_imag, real * turn_imag + imag * turn_real)
        for half in range(2):
            high, low = split(table[half])
            table_high_ref[:, half * CH : (half + 1) * CH] = high
            table_low_ref[:, half * CH : (half + 1) * CH] = low
        for block in range(CHUNK // LANES):
            here = slice(block * LANES, (block + 1) * LANES)
            lanes = slice(part * CHUNK + block * LANES, part * CHUNK + (block + 1) * LANES)
            taps = [jnp.broadcast_to(h_ref[t : t + 1, lanes], (ROWS, LANES)) for t in range(TAPS)]
            for row in range(0, inputs, ROWS):
                x = [ref[row : row + ROWS, lanes].astype(F32) for ref in x_refs]
                for s, products in enumerate(plan):
                    value = None
                    for t, frame in products:
                        product = taps[t] * x[frame]
                        value = product if value is None else value + product
                    high, low = split(value)
                    at = slice(s * inputs + row, s * inputs + row + ROWS)
                    high_ref[at, here] = high
                    low_ref[at, here] = low

    def contract(part):
        high_ref, low_ref, table_high_ref, table_low_ref = slots[part]
        dot = functools.partial(jnp.dot, preferred_element_type=F32)
        high = high_ref[...]
        table_high = table_high_ref[...]
        acc_ref[...] += dot(high, table_high) + dot(high, table_low_ref[...]) + dot(low_ref[...], table_high)

    fill(0)
    contract(1)
    fill(1)
    contract(0)

    @pl.when(step == pl.num_programs(0) - 1)
    def _():
        contract(1)
        for s in range(len(plan)):
            rows = slice(s * inputs, (s + 1) * inputs)
            pair = jnp.concatenate([acc_ref[rows, :CH], acc_ref[rows, CH:]], axis=0)
            out_ref[:, s, :] = pair.T
        for s in range(len(plan), frames):
            out_ref[:, s, :] = jnp.zeros((CH, 2 * inputs), F32)


def spectra(voltages, coefficients, carried):
    inputs, samples = voltages.shape
    frames = samples // NFFT
    small, base = twiddles()
    pair = 2 * CHUNK
    steps = NFFT // pair
    rows = len(terms(carried, frames)) * inputs
    frame_spec = lambda s: pl.BlockSpec((inputs, pair), lambda j: (0, s * steps + j))
    slot = [
        pltpu.VMEM((rows, CHUNK), BF16),
        pltpu.VMEM((rows, CHUNK), BF16),
        pltpu.VMEM((CHUNK, 2 * CH), BF16),
        pltpu.VMEM((CHUNK, 2 * CH), BF16),
    ]
    return pl.pallas_call(
        functools.partial(channelize, carried, frames, inputs),
        out_shape=jax.ShapeDtypeStruct((CH, frames, 2 * inputs), F32),
        grid=(steps,),
        in_specs=[frame_spec(s) for s in range(frames)]
        + [
            pl.BlockSpec((TAPS, pair), lambda j: (0, j)),
            pl.BlockSpec(small.shape, lambda j: (0, 0, 0)),
            pl.BlockSpec(base.shape, lambda j: (0, 0, 0)),
        ],
        out_specs=pl.BlockSpec((CH, frames, 2 * inputs), lambda j: (0, 0, 0)),
        scratch_shapes=slot + slot + [pltpu.VMEM((rows, 2 * CH), F32)],
        compiler_params=pltpu.CompilerParams(vmem_limit_bytes=48 * 2**20),
        cost_estimate=pl.CostEstimate(
            flops=6 * rows * NFFT * 2 * CH, bytes_accessed=2 * inputs * samples, transcendentals=0
        ),
        name="carried" if carried else "current",
    )(*[voltages] * frames, coefficients, small, base)


def correlate(n_time, n_input, inputs, frames, got_ref, out_ref, left_high, left_low, right_high, right_low):
    count = n_time * frames
    dot = functools.partial(jnp.dot, preferred_element_type=F32)

    @pl.when(pl.program_id(0) == 0)
    def _():
        for i in range(n_time):
            real_rows = slice(i * frames, (i + 1) * frames)
            imag_rows = slice(count + i * frames, count + (i + 1) * frames)
            for j in range(0, n_input, 2):
                lanes = slice(j * inputs, (j + 2) * inputs)
                first, second = got_ref[i * n_input + j], got_ref[i * n_input + j + 1]
                real = jnp.concatenate([first[:, :inputs], second[:, :inputs]], axis=1)
                imag = jnp.concatenate([first[:, inputs:], second[:, inputs:]], axis=1)
                real_high, real_low = split(real)
                imag_high, imag_low = split(imag)
                right_high[0, real_rows, lanes] = real_high
                right_low[0, real_rows, lanes] = real_low
                right_high[0, imag_rows, lanes] = imag_high
                right_low[0, imag_rows, lanes] = imag_low
                right_high[1, real_rows, lanes] = -imag_high
                right_low[1, real_rows, lanes] = -imag_low
                right_high[1, imag_rows, lanes] = real_high
                right_low[1, imag_rows, lanes] = real_low
        left_high[...] = right_high[0].T
        left_low[...] = right_low[0].T

    size = out_ref.shape[2]
    rows = pl.ds(pl.multiple_of(pl.program_id(0) * size, size), size)
    high, low = left_high[rows, :], left_low[rows, :]
    for part in range(2):
        total = dot(high, right_high[part]) + dot(high, right_low[part]) + dot(low, right_high[part])
        out_ref[part, 0] = total * (1.0 / count)


def visibilities(received, n_time, n_input):
    devices, frames, width = received.shape
    inputs = width // 2
    total = n_input * inputs
    depth = 2 * n_time * frames
    block = 128
    return pl.pallas_call(
        functools.partial(correlate, n_time, n_input, inputs, frames),
        out_shape=jax.ShapeDtypeStruct((2, 1, total, total), F32),
        grid=(total // block,),
        in_specs=[pl.BlockSpec(received.shape, lambda j: (0, 0, 0))],
        out_specs=pl.BlockSpec((2, 1, block, total), lambda j: (0, 0, j, 0)),
        scratch_shapes=[pltpu.VMEM((total, depth), BF16)] * 2 + [pltpu.VMEM((2, depth, total), BF16)] * 2,
        compiler_params=pltpu.CompilerParams(vmem_limit_bytes=48 * 2**20),
        name="correlate",
    )(received)


def shards(voltages, coefficients):
    n_time = lax.axis_size("tm")
    n_input = lax.axis_size("inp")
    carried = spectra(voltages, coefficients, True)
    arrived = lax.ppermute(carried, "tm", [(i, i + 1) for i in range(n_time - 1)])
    current = spectra(voltages, coefficients, False)
    outgoing = current + arrived
    received = lax.all_to_all(outgoing, ("tm", "inp"), split_axis=0, concat_axis=0, tiled=True)
    return visibilities(received, n_time, n_input)


def solution(mesh):
    in_specs = (P("inp", "tm"), P())
    out_specs = P(None, ("tm", "inp"), None, None)
    return jax.shard_map(shards, mesh=mesh, in_specs=in_specs, out_specs=out_specs, check_vma=False)
```

```python
import functools

import jax
import jax.numpy as jnp
import numpy as np
from jax import lax
from jax.experimental import pallas as pl
from jax.experimental.pallas import tpu as pltpu
from jax.sharding import PartitionSpec as P

NFFT = 8192
TAPS = 16
CH = 128
CH0 = 1024
LANES = 128
CHUNK = 256
HALF = NFFT // 2
GROUP = 8
DEPTH = 1
F32 = jnp.float32
BF16 = jnp.bfloat16


def twiddles():
    channel = (CH0 + np.arange(CH)).reshape(CH // 2, 2).T
    small = 2.0 * np.pi / NFFT * (np.arange(CHUNK)[:, None] * channel[:, None, :] % NFFT)
    base = 2.0 * np.pi / NFFT * (np.arange(HALF // CHUNK)[:, None, None] * CHUNK * channel % NFFT)
    real, imag = np.cos(small) * NFFT ** (-0.5), -np.sin(small) * NFFT ** (-0.5)
    turn_real, turn_imag = np.cos(base), -np.sin(base)
    small = np.stack([np.concatenate([real, imag], axis=-1), np.concatenate([-imag, real], axis=-1)])
    base = np.stack([np.concatenate([turn_real] * 2, axis=-1), np.concatenate([turn_imag] * 2, axis=-1)], axis=1)
    return jnp.asarray(small, F32), jnp.asarray(base, F32)


def split(value):
    high = value.astype(BF16)
    return high, (value - high.astype(F32)).astype(BF16)


def toeplitz_tree(coefficients, depth):
    size = (len(coefficients) + 1) // 2
    if depth == 0 or size == 1:
        return coefficients
    half = size // 2
    upper, middle, lower = (coefficients[k : k + size - 1] for k in (0, half, size))
    above = [a - b for a, b in zip(upper, middle)]
    below = [a - b for a, b in zip(lower, middle)]
    return [toeplitz_tree(part, depth - 1) for part in (middle, above, below)]


def flatten(tree):
    return [leaf for part in tree for leaf in flatten(part)] if isinstance(tree, list) else [tree]


def rebuild(tree, leaves):
    return [rebuild(part, leaves) for part in tree] if isinstance(tree, list) else next(leaves)


def weighted(pairs):
    total = None
    for coefficient, sample in pairs:
        product = coefficient * sample
        total = product if total is None else total + product
    return total


def toeplitz(tree, samples):
    size = len(samples)
    if len(tree) == 2 * size - 1 and not isinstance(tree[0], list):
        return [weighted((tree[size - 1 + i - j], samples[j]) for j in range(size)) for i in range(size)]
    half = size // 2
    first, second = samples[:half], samples[half:]
    both = toeplitz(tree[0], [a + b for a, b in zip(first, second)])
    above = toeplitz(tree[1], second)
    below = toeplitz(tree[2], first)
    return [a + b for a, b in zip(both, above)] + [a + b for a, b in zip(both, below)]


def coefficient_tree(taps):
    half = TAPS // 2
    return [list(taps), toeplitz_tree(list(taps[1:]), DEPTH)]


def later_frames(tree, x):
    taps, middle = tree
    half = TAPS // 2
    inner = toeplitz(middle, x[half:])
    first = [weighted((taps[TAPS + s - j], x[j]) for j in range(s + 1, half)) for s in range(half - 1)]
    second = [weighted((taps[TAPS + s - j], x[j + half]) for j in range(s + 1, half)) for s in range(half - 1)]
    return [a + b for a, b in zip(inner, first)] + [inner[half - 1]] + second


def these_frames(tree, x):
    taps, middle = tree
    half = TAPS // 2
    inner = toeplitz(middle, x[:half])
    first = [weighted((taps[s - j], x[j]) for j in range(s + 1)) for s in range(half)]
    second = [weighted((taps[s - j], x[j + half]) for j in range(s + 1)) for s in range(half)]
    return first + [a + b for a, b in zip(second, inner)]


def channelize(carried, frames, inputs, *refs):
    x_refs = refs[:frames], refs[frames : 2 * frames]
    h_refs, (small_ref, base_ref, out_ref, acc_ref) = refs[2 * frames : 2 * frames + 2], refs[2 * frames + 2 :]
    step = pl.program_id(0)
    groups = inputs // GROUP

    @pl.when(step == 0)
    def _():
        acc_ref[...] = jnp.zeros_like(acc_ref)

    lines = [[], []]
    trees = []
    for block in range(CHUNK // LANES):
        lanes = slice(block * LANES, (block + 1) * LANES)
        trees.append([])
        for h_ref in h_refs:
            taps = [jnp.broadcast_to(h_ref[t : t + 1, lanes], (GROUP, LANES)) for t in range(TAPS)]
            trees[-1].append(coefficient_tree(taps))
    for group in range(groups):
        at = slice(group * GROUP, (group + 1) * GROUP)
        columns = [[], []]
        for block in range(CHUNK // LANES):
            lanes = slice(block * LANES, (block + 1) * LANES)
            first, second = (
                (later_frames if carried else these_frames)(tree, [ref[at, lanes].astype(F32) for ref in x])
                for tree, x in zip(trees[block], x_refs)
            )
            for parity in range(2):
                values = [a - b if parity else a + b for a, b in zip(first, second)]
                if carried:
                    values.append(jnp.zeros((GROUP, LANES), F32))
                pieces = [split(jnp.concatenate(values[s : s + 2], axis=0)) for s in range(0, frames, 2)]
                columns[parity].append(
                    jnp.concatenate([p[0] for p in pieces] + [p[1] for p in pieces], axis=0)
                )
        for parity in range(2):
            lines[parity].append(jnp.concatenate(columns[parity], axis=1))

    for parity in range(2):
        table = small_ref[0, parity] * base_ref[step, 0, parity : parity + 1]
        table = table + small_ref[1, parity] * base_ref[step, 1, parity : parity + 1]
        total = jnp.dot(
            jnp.concatenate(lines[parity], axis=0),
            jnp.concatenate(split(table), axis=1),
            preferred_element_type=F32,
        )
        rows = frames * GROUP
        for group in range(groups):
            high = total[2 * group * rows : (2 * group + 1) * rows]
            low = total[(2 * group + 1) * rows : (2 * group + 2) * rows]
            acc_ref[parity, group * rows : (group + 1) * rows] += high + low

    @pl.when(step == pl.num_programs(0) - 1)
    def _():
        half = CH // 2
        for s in range(frames):
            sums = []
            for parity in range(2):
                starts = [(group * frames + s) * GROUP for group in range(groups)]
                whole = jnp.concatenate([acc_ref[parity, start : start + GROUP] for start in starts], axis=0)
                sums.append(whole[:, :CH] + whole[:, CH:])
            real = jnp.concatenate([part[:, :half] for part in sums], axis=1)
            imag = jnp.concatenate([part[:, half:] for part in sums], axis=1)
            turned = jnp.concatenate([real, imag], axis=0).T
            for parity in range(2):
                out_ref[:, parity, s, :] = turned[parity * half : (parity + 1) * half]


def spectra(voltages, coefficients, carried):
    inputs, samples = voltages.shape
    frames = samples // NFFT
    small, base = twiddles()
    steps = HALF // CHUNK
    rows = frames * inputs
    frame_spec = lambda s, part: pl.BlockSpec((inputs, CHUNK), lambda j: (0, (2 * s + part) * steps + j))
    out = pl.pallas_call(
        functools.partial(channelize, carried, frames, inputs),
        out_shape=jax.ShapeDtypeStruct((CH // 2, 2, frames, 2 * inputs), F32),
        grid=(steps,),
        in_specs=[frame_spec(s, part) for part in range(2) for s in range(frames)]
        + [
            pl.BlockSpec((TAPS, CHUNK), lambda j: (0, j)),
            pl.BlockSpec((TAPS, CHUNK), lambda j: (0, steps + j)),
            pl.BlockSpec(small.shape, lambda j: (0, 0, 0, 0)),
            pl.BlockSpec(base.shape, lambda j: (0, 0, 0, 0)),
        ],
        out_specs=pl.BlockSpec((CH // 2, 2, frames, 2 * inputs), lambda j: (0, 0, 0, 0)),
        scratch_shapes=[pltpu.VMEM((2, rows, 2 * CH), F32)],
        compiler_params=pltpu.CompilerParams(vmem_limit_bytes=48 * 2**20),
        cost_estimate=pl.CostEstimate(
            flops=4 * rows * NFFT * 2 * CH, bytes_accessed=2 * inputs * samples, transcendentals=0
        ),
        name="carried" if carried else "current",
    )(*[voltages] * (2 * frames), coefficients, coefficients, small, base)
    return out.reshape(CH, frames, 2 * inputs)


def correlate(n_time, n_input, inputs, frames, got_ref, out_ref, left_high, left_low, right_high, right_low):
    count = n_time * frames
    dot = functools.partial(jnp.dot, preferred_element_type=F32)

    @pl.when(pl.program_id(0) == 0)
    def _():
        for i in range(n_time):
            real_rows = slice(i * frames, (i + 1) * frames)
            imag_rows = slice(count + i * frames, count + (i + 1) * frames)
            for j in range(0, n_input, 2):
                lanes = slice(j * inputs, (j + 2) * inputs)
                first, second = got_ref[i * n_input + j], got_ref[i * n_input + j + 1]
                real = jnp.concatenate([first[:, :inputs], second[:, :inputs]], axis=1)
                imag = jnp.concatenate([first[:, inputs:], second[:, inputs:]], axis=1)
                real_high, real_low = split(real)
                imag_high, imag_low = split(imag)
                right_high[0, real_rows, lanes] = real_high
                right_low[0, real_rows, lanes] = real_low
                right_high[0, imag_rows, lanes] = imag_high
                right_low[0, imag_rows, lanes] = imag_low
                right_high[1, real_rows, lanes] = -imag_high
                right_low[1, real_rows, lanes] = -imag_low
                right_high[1, imag_rows, lanes] = real_high
                right_low[1, imag_rows, lanes] = real_low
        left_high[...] = right_high[0].T
        left_low[...] = right_low[0].T

    size = out_ref.shape[2]
    rows = pl.ds(pl.multiple_of(pl.program_id(0) * size, size), size)
    high, low = left_high[rows, :], left_low[rows, :]
    for part in range(2):
        total = dot(high, right_high[part]) + dot(high, right_low[part]) + dot(low, right_high[part])
        out_ref[part, 0] = total * (1.0 / count)


def visibilities(received, n_time, n_input):
    devices, frames, width = received.shape
    inputs = width // 2
    total = n_input * inputs
    depth = 2 * n_time * frames
    block = 128
    return pl.pallas_call(
        functools.partial(correlate, n_time, n_input, inputs, frames),
        out_shape=jax.ShapeDtypeStruct((2, 1, total, total), F32),
        grid=(total // block,),
        in_specs=[pl.BlockSpec(received.shape, lambda j: (0, 0, 0))],
        out_specs=pl.BlockSpec((2, 1, block, total), lambda j: (0, 0, j, 0)),
        scratch_shapes=[pltpu.VMEM((total, depth), BF16)] * 2 + [pltpu.VMEM((2, depth, total), BF16)] * 2,
        compiler_params=pltpu.CompilerParams(vmem_limit_bytes=48 * 2**20),
        name="correlate",
    )(received)


def shards(voltages, coefficients):
    n_time = lax.axis_size("tm")
    n_input = lax.axis_size("inp")
    carried = spectra(voltages, coefficients, True)
    arrived = lax.ppermute(carried, "tm", [(i, i + 1) for i in range(n_time - 1)])
    current = spectra(voltages, coefficients, False)
    outgoing = current + arrived
    received = lax.all_to_all(outgoing, ("tm", "inp"), split_axis=0, concat_axis=0, tiled=True)
    return visibilities(received, n_time, n_input)


def solution(mesh):
    in_specs = (P("inp", "tm"), P())
    out_specs = P(None, ("tm", "inp"), None, None)
    return jax.shard_map(shards, mesh=mesh, in_specs=in_specs, out_specs=out_specs, check_vma=False)
```

```python
import functools

import jax
import jax.numpy as jnp
import numpy as np
from jax import lax
from jax.experimental import pallas as pl
from jax.experimental.pallas import tpu as pltpu
from jax.sharding import PartitionSpec as P

NFFT = 8192
TAPS = 16
CH = 128
CH0 = 1024
LANES = 128
CHUNK = 512
HALF = NFFT // 2
GROUP = 8
FINE = 16
DEPTH = 2
F32 = jnp.float32
BF16 = jnp.bfloat16


def turns(samples):
    channel = (CH0 + np.arange(CH)).reshape(CH // 2, 2).T
    angle = 2.0 * np.pi / NFFT * (samples[:, None, None] * channel % NFFT)
    return np.cos(angle), -np.sin(angle)


def twiddles():
    real, imag = (part.transpose(1, 0, 2) * NFFT ** (-0.5) for part in turns(np.arange(FINE)))
    fine = np.stack([np.concatenate([real, imag], axis=-1), np.concatenate([-imag, real], axis=-1)])
    coarse, base = (
        np.stack([np.concatenate([part] * 2, axis=-1) for part in turns(samples)], axis=1)
        for samples in (np.arange(0, CHUNK, FINE), np.arange(0, HALF, CHUNK))
    )
    return jnp.asarray(np.concatenate([part.reshape(-1, CH) for part in (fine, coarse, base)]), F32)


def split(value):
    high = value.astype(BF16)
    return high, (value - high.astype(F32)).astype(BF16)


def toeplitz_tree(coefficients, depth):
    size = (len(coefficients) + 1) // 2
    if depth == 0 or size == 1:
        return coefficients
    half = size // 2
    upper, middle, lower = (coefficients[k : k + size - 1] for k in (0, half, size))
    above = [a - b for a, b in zip(upper, middle)]
    below = [a - b for a, b in zip(lower, middle)]
    return [toeplitz_tree(part, depth - 1) for part in (middle, above, below)]


def flatten(tree):
    return [leaf for part in tree for leaf in flatten(part)] if isinstance(tree, list) else [tree]


def rebuild(tree, leaves):
    return [rebuild(part, leaves) for part in tree] if isinstance(tree, list) else next(leaves)


def weighted(pairs):
    parts = [coefficient * sample for coefficient, sample in pairs]
    while len(parts) > 1:
        parts = [parts[k] + parts[k + 1] if k + 1 < len(parts) else parts[k] for k in range(0, len(parts), 2)]
    return parts[0]


def toeplitz(tree, samples):
    size = len(samples)
    if len(tree) == 2 * size - 1 and not isinstance(tree[0], list):
        return [weighted((tree[size - 1 + i - j], samples[j]) for j in range(size)) for i in range(size)]
    half = size // 2
    first, second = samples[:half], samples[half:]
    both = toeplitz(tree[0], [a + b for a, b in zip(first, second)])
    above = toeplitz(tree[1], second)
    below = toeplitz(tree[2], first)
    return [a + b for a, b in zip(both, above)] + [a + b for a, b in zip(both, below)]


def coefficient_tree(taps):
    half = TAPS // 2
    return [list(taps), toeplitz_tree(list(taps[1:]), DEPTH)]


def later_frames(tree, x):
    taps, middle = tree
    half = TAPS // 2
    inner = toeplitz(middle, x[half:])
    first = [weighted((taps[TAPS + s - j], x[j]) for j in range(s + 1, half)) for s in range(half - 1)]
    second = [weighted((taps[TAPS + s - j], x[j + half]) for j in range(s + 1, half)) for s in range(half - 1)]
    return [a + b for a, b in zip(inner, first)] + [inner[half - 1]] + second


def these_frames(tree, x):
    taps, middle = tree
    half = TAPS // 2
    inner = toeplitz(middle, x[:half])
    first = [weighted((taps[s - j], x[j]) for j in range(s + 1)) for s in range(half)]
    second = [weighted((taps[s - j], x[j + half]) for j in range(s + 1)) for s in range(half)]
    return first + [a + b for a, b in zip(second, inner)]


def channelize(carried, frames, inputs, x_ref, h_first, h_second, table_ref, out_ref, acc_ref, small_ref):
    h_refs = h_first, h_second
    step = pl.program_id(0)
    groups = inputs // GROUP
    turn = lambda start, part, parity: table_ref[pl.ds(start + 2 * part + parity, 1), :]

    @pl.when(step == 0)
    def _():
        acc_ref[...] = jnp.zeros_like(acc_ref)
        for parity in range(2):
            real, imag = (table_ref[(2 * part + parity) * FINE : (2 * part + parity + 1) * FINE] for part in range(2))
            for k in range(CHUNK // FINE):
                at = slice(k * FINE, (k + 1) * FINE)
                turn_real, turn_imag = (turn(4 * FINE + 4 * k, part, parity) for part in range(2))
                small_ref[0, parity, at] = real * turn_real + imag * turn_imag
                small_ref[1, parity, at] = imag * turn_real - real * turn_imag

    lines = [[], []]
    trees = []
    for block in range(CHUNK // LANES):
        lanes = slice(block * LANES, (block + 1) * LANES)
        trees.append([])
        for h_ref in h_refs:
            taps = [jnp.broadcast_to(h_ref[t : t + 1, lanes], (GROUP, LANES)) for t in range(TAPS)]
            trees[-1].append(coefficient_tree(taps))
    for group in range(groups):
        columns = [[], []]
        for block in range(CHUNK // LANES):
            first, second = (
                (later_frames if carried else these_frames)(
                    trees[block][part], [x_ref[group, s, part, block].astype(F32) for s in range(frames)]
                )
                for part in range(2)
            )
            for parity in range(2):
                values = [a - b if parity else a + b for a, b in zip(first, second)]
                if carried:
                    values.append(jnp.zeros((GROUP, LANES), F32))
                pieces = [split(jnp.concatenate(values[s : s + 2], axis=0)) for s in range(0, frames, 2)]
                columns[parity].append(
                    jnp.concatenate([p[0] for p in pieces] + [p[1] for p in pieces], axis=0)
                )
        for parity in range(2):
            lines[parity].append(jnp.concatenate(columns[parity], axis=1))

    for parity in range(2):
        start = 4 * FINE + 4 * (CHUNK // FINE) + 4 * step
        table = small_ref[0, parity] * turn(start, 0, parity) + small_ref[1, parity] * turn(start, 1, parity)
        total = jnp.dot(
            jnp.concatenate(lines[parity], axis=0),
            jnp.concatenate(split(table), axis=1),
            preferred_element_type=F32,
        )
        rows = frames * GROUP
        for group in range(groups):
            high = total[2 * group * rows : (2 * group + 1) * rows]
            low = total[(2 * group + 1) * rows : (2 * group + 2) * rows]
            acc_ref[parity, group * rows : (group + 1) * rows] += high + low

    @pl.when(step == pl.num_programs(0) - 1)
    def _():
        for parity in range(2):
            out_ref[parity] = acc_ref[parity, :, :CH] + acc_ref[parity, :, CH:]


def assemble(frames, inputs, here_ref, before_ref, out_ref):
    groups = inputs // GROUP
    half = CH // 2
    for s in range(frames):
        sums = []
        for parity in range(2):
            spans = [slice((group * frames + s) * GROUP, (group * frames + s + 1) * GROUP) for group in range(groups)]
            sums.append(
                jnp.concatenate([here_ref[parity, span] + before_ref[parity, span] for span in spans], axis=0)
            )
        real = jnp.concatenate([part[:, :half] for part in sums], axis=1)
        imag = jnp.concatenate([part[:, half:] for part in sums], axis=1)
        turned = jnp.concatenate([real, imag], axis=0).T
        for parity in range(2):
            out_ref[:, parity, s, :] = turned[parity * half : (parity + 1) * half]


def messages(here, before, inputs):
    frames = here.shape[1] // inputs
    return pl.pallas_call(
        functools.partial(assemble, frames, inputs),
        out_shape=jax.ShapeDtypeStruct((CH // 2, 2, frames, 2 * inputs), F32),
        compiler_params=pltpu.CompilerParams(vmem_limit_bytes=16 * 2**20),
        name="messages",
    )(here, before).reshape(CH, frames, 2 * inputs)


def spectra(voltages, coefficients, carried):
    inputs, samples = voltages.shape
    frames = samples // NFFT
    table, coefficients = (pltpu.with_memory_space_constraint(part, pltpu.HBM) for part in (twiddles(), coefficients))
    steps = HALF // CHUNK
    rows = frames * inputs
    tiles = voltages.reshape(inputs // GROUP, GROUP, samples // LANES, LANES).transpose(0, 2, 1, 3)
    tiles = tiles.reshape(inputs // GROUP, frames, 2, HALF // LANES, GROUP, LANES)
    block = (inputs // GROUP, frames, 2, CHUNK // LANES, GROUP, LANES)
    return pl.pallas_call(
        functools.partial(channelize, carried, frames, inputs),
        out_shape=jax.ShapeDtypeStruct((2, rows, CH), F32),
        grid=(steps,),
        in_specs=[
            pl.BlockSpec(block, lambda j: (0, 0, 0, j, 0, 0)),
            pl.BlockSpec((TAPS, CHUNK), lambda j: (0, j)),
            pl.BlockSpec((TAPS, CHUNK), lambda j: (0, steps + j)),
            pl.BlockSpec(table.shape, lambda j: (0, 0)),
        ],
        out_specs=pl.BlockSpec((2, rows, CH), lambda j: (0, 0, 0)),
        scratch_shapes=[pltpu.VMEM((2, rows, 2 * CH), F32), pltpu.VMEM((2, 2, CHUNK, CH), F32)],
        compiler_params=pltpu.CompilerParams(vmem_limit_bytes=48 * 2**20),
        cost_estimate=pl.CostEstimate(
            flops=4 * rows * NFFT * 2 * CH, bytes_accessed=2 * inputs * samples, transcendentals=0
        ),
        name="carried" if carried else "current",
    )(tiles, coefficients, coefficients, table)


def correlate(n_time, n_input, inputs, frames, got_ref, out_ref, left_high, left_low, right_high, right_low):
    count = n_time * frames
    dot = functools.partial(jnp.dot, preferred_element_type=F32)

    @pl.when(pl.program_id(0) == 0)
    def _():
        for i in range(n_time):
            real_rows = slice(i * frames, (i + 1) * frames)
            imag_rows = slice(count + i * frames, count + (i + 1) * frames)
            for j in range(0, n_input, 2):
                lanes = slice(j * inputs, (j + 2) * inputs)
                first, second = got_ref[i * n_input + j], got_ref[i * n_input + j + 1]
                real = jnp.concatenate([first[:, :inputs], second[:, :inputs]], axis=1)
                imag = jnp.concatenate([first[:, inputs:], second[:, inputs:]], axis=1)
                real_high, real_low = split(real)
                imag_high, imag_low = split(imag)
                right_high[0, real_rows, lanes] = real_high
                right_low[0, real_rows, lanes] = real_low
                right_high[0, imag_rows, lanes] = imag_high
                right_low[0, imag_rows, lanes] = imag_low
                right_high[1, real_rows, lanes] = -imag_high
                right_low[1, real_rows, lanes] = -imag_low
                right_high[1, imag_rows, lanes] = real_high
                right_low[1, imag_rows, lanes] = real_low
        left_high[...] = right_high[0].T
        left_low[...] = right_low[0].T

    size = out_ref.shape[2]
    rows = pl.ds(pl.multiple_of(pl.program_id(0) * size, size), size)
    high, low = left_high[rows, :], left_low[rows, :]
    for part in range(2):
        total = dot(high, right_high[part]) + dot(high, right_low[part]) + dot(low, right_high[part])
        out_ref[part, 0] = total * (1.0 / count)


def visibilities(received, n_time, n_input):
    devices, frames, width = received.shape
    inputs = width // 2
    total = n_input * inputs
    depth = 2 * n_time * frames
    block = 128
    return pl.pallas_call(
        functools.partial(correlate, n_time, n_input, inputs, frames),
        out_shape=jax.ShapeDtypeStruct((2, 1, total, total), F32),
        grid=(total // block,),
        in_specs=[pl.BlockSpec(received.shape, lambda j: (0, 0, 0))],
        out_specs=pl.BlockSpec((2, 1, block, total), lambda j: (0, 0, j, 0)),
        scratch_shapes=[pltpu.VMEM((total, depth), BF16)] * 2 + [pltpu.VMEM((2, depth, total), BF16)] * 2,
        compiler_params=pltpu.CompilerParams(vmem_limit_bytes=48 * 2**20),
        name="correlate",
    )(received)


def shards(voltages, coefficients):
    n_time = lax.axis_size("tm")
    n_input = lax.axis_size("inp")
    carried = spectra(voltages, coefficients, True)
    arrived = lax.ppermute(carried, "tm", [(i, i + 1) for i in range(n_time - 1)])
    current = spectra(voltages, coefficients, False)
    outgoing = messages(current, arrived, voltages.shape[0])
    received = lax.all_to_all(outgoing, ("tm", "inp"), split_axis=0, concat_axis=0, tiled=True)
    return visibilities(received, n_time, n_input)


def solution(mesh):
    in_specs = (P("inp", "tm"), P())
    out_specs = P(None, ("tm", "inp"), None, None)
    return jax.shard_map(shards, mesh=mesh, in_specs=in_specs, out_specs=out_specs, check_vma=False)
```

```python
import functools

import jax
import jax.numpy as jnp
import numpy as np
from jax import lax
from jax.experimental import pallas as pl
from jax.experimental.pallas import tpu as pltpu
from jax.sharding import PartitionSpec as P

NFFT = 8192
TAPS = 16
CH = 128
CH0 = 1024
LANES = 128
CHUNK = 512
HALF = NFFT // 2
GROUP = 8
FINE = 16
TILE = 512
SPAN = 8
DEPTH = 2
F32 = jnp.float32
BF16 = jnp.bfloat16


def turns(samples):
    channel = (CH0 + np.arange(CH)).reshape(CH // 2, 2).T
    angle = 2.0 * np.pi / NFFT * (samples[:, None, None] * channel % NFFT)
    return np.cos(angle), -np.sin(angle)


def twiddles():
    real, imag = (part.transpose(1, 0, 2) * NFFT ** (-0.5) for part in turns(np.arange(FINE)))
    fine = np.stack([np.concatenate([real, imag], axis=-1), np.concatenate([-imag, real], axis=-1)])
    coarse, base = (
        np.stack([np.concatenate([part] * 2, axis=-1) for part in turns(samples)], axis=1)
        for samples in (np.arange(0, CHUNK, FINE), np.arange(0, HALF, CHUNK))
    )
    return jnp.asarray(np.concatenate([part.reshape(-1, CH) for part in (fine, coarse, base)]), F32)


def split(value):
    high = value.astype(BF16)
    return high, (value - high.astype(F32)).astype(BF16)


def toeplitz_tree(coefficients, depth):
    size = (len(coefficients) + 1) // 2
    if depth == 0 or size == 1:
        return coefficients
    half = size // 2
    upper, middle, lower = (coefficients[k : k + size - 1] for k in (0, half, size))
    above = [a - b for a, b in zip(upper, middle)]
    below = [a - b for a, b in zip(lower, middle)]
    return [toeplitz_tree(part, depth - 1) for part in (middle, above, below)]


def weighted(pairs):
    parts = [coefficient * sample for coefficient, sample in pairs]
    while len(parts) > 1:
        parts = [parts[k] + parts[k + 1] if k + 1 < len(parts) else parts[k] for k in range(0, len(parts), 2)]
    return parts[0]


def toeplitz(tree, samples):
    size = len(samples)
    if len(tree) == 2 * size - 1 and not isinstance(tree[0], list):
        return [weighted((tree[size - 1 + i - j], samples[j]) for j in range(size)) for i in range(size)]
    half = size // 2
    first, second = samples[:half], samples[half:]
    both = toeplitz(tree[0], [a + b for a, b in zip(first, second)])
    above = toeplitz(tree[1], second)
    below = toeplitz(tree[2], first)
    return [a + b for a, b in zip(both, above)] + [a + b for a, b in zip(both, below)]


def coefficient_tree(taps):
    half = TAPS // 2
    taps = list(taps)
    near = toeplitz_tree(taps[1:half], DEPTH - 1)
    far = toeplitz_tree(taps[half + 1 :], DEPTH - 1)
    return taps, near, toeplitz_tree(taps[1:], DEPTH), far


def added(first, second):
    return [a + b for a, b in zip(first, second)]


def lower(taps, near, x):
    quarter = TAPS // 4
    inner = toeplitz(near, x[:quarter])
    first, second = (
        [weighted((taps[s - j], part[j]) for j in range(s + 1)) for s in range(quarter)]
        for part in (x[:quarter], x[quarter:])
    )
    return first + added(inner, second)


def upper(taps, far, x):
    quarter = TAPS // 4
    inner = toeplitz(far, x[quarter:])
    first, second = (
        [weighted((taps[TAPS + s - j], part[j]) for j in range(s + 1, quarter)) for s in range(quarter - 1)]
        for part in (x[:quarter], x[quarter:])
    )
    return added(inner, first) + inner[quarter - 1 :] + second


def later_frames(tree, x):
    taps, near, middle, far = tree
    half = TAPS // 2
    inner = toeplitz(middle, x[half:])
    return added(inner, upper(taps, far, x[:half])) + inner[half - 1 :] + upper(taps, far, x[half:])


def these_frames(tree, x):
    taps, near, middle, far = tree
    half = TAPS // 2
    inner = toeplitz(middle, x[:half])
    return lower(taps, near, x[:half]) + added(inner, lower(taps, near, x[half:]))


def channelize(carried, frames, inputs, x_ref, h_first, h_second, *refs):
    h_refs = h_first, h_second
    step = pl.program_id(0)
    groups = inputs // GROUP
    if carried:
        twiddle_ref, out_ref, table_ref, small_ref = refs
        turn = lambda start, part, parity: twiddle_ref[pl.ds(start + 2 * part + parity, 1), :]
    else:
        table_ref, out_ref = refs

    @pl.when(step == 0)
    def _():
        out_ref[...] = jnp.zeros_like(out_ref)
        if not carried:
            return
        for parity in range(2):
            starts = [(2 * part + parity) * FINE for part in range(2)]
            real, imag = (twiddle_ref[start : start + FINE] for start in starts)
            for k in range(CHUNK // FINE):
                at = slice(k * FINE, (k + 1) * FINE)
                turn_real, turn_imag = (turn(4 * FINE + 4 * k, part, parity) for part in range(2))
                small_ref[0, parity, at] = real * turn_real + imag * turn_imag
                small_ref[1, parity, at] = imag * turn_real - real * turn_imag

    lines = []
    trees = []
    for block in range(CHUNK // LANES):
        lanes = slice(block * LANES, (block + 1) * LANES)
        trees.append([])
        for h_ref in h_refs:
            taps = [jnp.broadcast_to(h_ref[t : t + 1, lanes], (GROUP, LANES)) for t in range(TAPS)]
            trees[-1].append(coefficient_tree(taps))
    width = TILE // LANES
    for tile in range(CHUNK // TILE):
        lines.append([[], []])
        for group in range(groups):
            columns = [[], []]
            for block in range(tile * width, (tile + 1) * width):
                first, second = (
                    (later_frames if carried else these_frames)(
                        trees[block][part], [x_ref[group, s, part, block].astype(F32) for s in range(frames)]
                    )
                    for part in range(2)
                )
                for parity in range(2):
                    values = [a - b if parity else a + b for a, b in zip(first, second)]
                    if carried:
                        values.append(jnp.zeros((GROUP, LANES), F32))
                    pieces = [split(jnp.concatenate(values[s : s + 2], axis=0)) for s in range(0, frames, 2)]
                    columns[parity].append([jnp.concatenate(part, axis=0) for part in zip(*pieces)])
            for parity in range(2):
                lines[tile][parity].append([jnp.concatenate(part, axis=1) for part in zip(*columns[parity])])

    rows = frames * GROUP
    here = pl.ds(pl.multiple_of(step * CHUNK, CHUNK), CHUNK)
    for parity in range(2):
        if carried:
            start = 4 * FINE + 4 * (CHUNK // FINE) + 4 * step
            wave = small_ref[0, parity] * turn(start, 0, parity) + small_ref[1, parity] * turn(start, 1, parity)
            table = jnp.concatenate(split(wave), axis=1)
            table_ref[parity, here] = table
        else:
            table = table_ref[parity, here]
        total = None
        for tile in range(CHUNK // TILE):
            line = lines[tile][parity]
            order = [line[first + k][part] for first in range(0, groups, SPAN) for part in range(2) for k in range(SPAN)]
            product = jnp.dot(
                jnp.concatenate(order, axis=0),
                table[tile * TILE : (tile + 1) * TILE],
                preferred_element_type=F32,
            )
            total = product if total is None else total + product
        for group in range(groups):
            place = 2 * (group // SPAN) * SPAN + group % SPAN
            both = total[place * rows : (place + 1) * rows] + total[(place + SPAN) * rows : (place + SPAN + 1) * rows]
            out_ref[parity, group * rows : (group + 1) * rows] += both[:, :CH] + both[:, CH:]


def assemble(frames, inputs, here_ref, before_ref, out_ref):
    groups = inputs // GROUP
    half = CH // 2
    for s in range(frames):
        sums = []
        for parity in range(2):
            spans = [slice((group * frames + s) * GROUP, (group * frames + s + 1) * GROUP) for group in range(groups)]
            sums.append(
                jnp.concatenate([here_ref[parity, span] + before_ref[parity, span] for span in spans], axis=0)
            )
        real = jnp.concatenate([part[:, :half] for part in sums], axis=1)
        imag = jnp.concatenate([part[:, half:] for part in sums], axis=1)
        turned = jnp.concatenate([real, imag], axis=0).T
        for parity in range(2):
            out_ref[:, parity, s, :] = turned[parity * half : (parity + 1) * half]


def messages(here, before, inputs):
    frames = here.shape[1] // inputs
    return pl.pallas_call(
        functools.partial(assemble, frames, inputs),
        out_shape=jax.ShapeDtypeStruct((CH // 2, 2, frames, 2 * inputs), F32),
        compiler_params=pltpu.CompilerParams(vmem_limit_bytes=16 * 2**20),
        name="messages",
    )(here, before).reshape(CH, frames, 2 * inputs)


def spectra(voltages, coefficients, table=None):
    inputs, samples = voltages.shape
    frames = samples // NFFT
    steps = HALF // CHUNK
    rows = frames * inputs
    coefficients = pltpu.with_memory_space_constraint(coefficients, pltpu.HBM)
    tiles = voltages.reshape(inputs // GROUP, GROUP, samples // LANES, LANES).transpose(0, 2, 1, 3)
    tiles = tiles.reshape(inputs // GROUP, frames, 2, HALF // LANES, GROUP, LANES)
    block = (inputs // GROUP, frames, 2, CHUNK // LANES, GROUP, LANES)
    in_specs = [
        pl.BlockSpec(block, lambda j: (0, 0, 0, j, 0, 0)),
        pl.BlockSpec((TAPS, CHUNK), lambda j: (0, j)),
        pl.BlockSpec((TAPS, CHUNK), lambda j: (0, steps + j)),
    ]
    out_shape = jax.ShapeDtypeStruct((2, rows, CH), F32)
    whole = pl.BlockSpec(memory_space=pltpu.VMEM)
    options = dict(
        grid=(steps,),
        compiler_params=pltpu.CompilerParams(vmem_limit_bytes=48 * 2**20),
        cost_estimate=pl.CostEstimate(
            flops=4 * rows * NFFT * 2 * CH, bytes_accessed=2 * inputs * samples, transcendentals=0
        ),
    )
    if table is not None:
        return pl.pallas_call(
            functools.partial(channelize, False, frames, inputs),
            out_shape=out_shape,
            in_specs=in_specs + [whole],
            out_specs=whole,
            name="current",
            **options,
        )(tiles, coefficients, coefficients, table)
    waves = pltpu.with_memory_space_constraint(twiddles(), pltpu.HBM)
    return pl.pallas_call(
        functools.partial(channelize, True, frames, inputs),
        out_shape=(out_shape, jax.ShapeDtypeStruct((2, HALF, 2 * CH), BF16)),
        in_specs=in_specs + [pl.BlockSpec(waves.shape, lambda j: (0, 0))],
        out_specs=(whole, whole),
        scratch_shapes=[pltpu.VMEM((2, 2, CHUNK, CH), F32)],
        name="carried",
        **options,
    )(tiles, coefficients, coefficients, waves)


def correlate(n_time, n_input, inputs, frames, got_ref, out_ref, left_high, left_low, right_high, right_low):
    count = n_time * frames
    dot = functools.partial(jnp.dot, preferred_element_type=F32)

    @pl.when(pl.program_id(0) == 0)
    def _():
        for i in range(n_time):
            real_rows = slice(i * frames, (i + 1) * frames)
            imag_rows = slice(count + i * frames, count + (i + 1) * frames)
            for j in range(0, n_input, 2):
                lanes = slice(j * inputs, (j + 2) * inputs)
                first, second = got_ref[i * n_input + j], got_ref[i * n_input + j + 1]
                real = jnp.concatenate([first[:, :inputs], second[:, :inputs]], axis=1)
                imag = jnp.concatenate([first[:, inputs:], second[:, inputs:]], axis=1)
                real_high, real_low = split(real)
                imag_high, imag_low = split(imag)
                right_high[0, real_rows, lanes] = real_high
                right_low[0, real_rows, lanes] = real_low
                right_high[0, imag_rows, lanes] = imag_high
                right_low[0, imag_rows, lanes] = imag_low
                right_high[1, real_rows, lanes] = -imag_high
                right_low[1, real_rows, lanes] = -imag_low
                right_high[1, imag_rows, lanes] = real_high
                right_low[1, imag_rows, lanes] = real_low
        left_high[...] = right_high[0].T
        left_low[...] = right_low[0].T

    size = out_ref.shape[2]
    rows = pl.ds(pl.multiple_of(pl.program_id(0) * size, size), size)
    high, low = left_high[rows, :], left_low[rows, :]
    for part in range(2):
        total = dot(high, right_high[part]) + dot(high, right_low[part]) + dot(low, right_high[part])
        out_ref[part, 0] = total * (1.0 / count)


def visibilities(received, n_time, n_input):
    devices, frames, width = received.shape
    inputs = width // 2
    total = n_input * inputs
    depth = 2 * n_time * frames
    block = 256
    return pl.pallas_call(
        functools.partial(correlate, n_time, n_input, inputs, frames),
        out_shape=jax.ShapeDtypeStruct((2, 1, total, total), F32),
        grid=(total // block,),
        in_specs=[pl.BlockSpec(memory_space=pltpu.VMEM)],
        out_specs=pl.BlockSpec((2, 1, block, total), lambda j: (0, 0, j, 0)),
        scratch_shapes=[pltpu.VMEM((total, depth), BF16)] * 2 + [pltpu.VMEM((2, depth, total), BF16)] * 2,
        compiler_params=pltpu.CompilerParams(vmem_limit_bytes=48 * 2**20),
        name="correlate",
    )(received)


def shards(voltages, coefficients):
    n_time = lax.axis_size("tm")
    n_input = lax.axis_size("inp")
    carried, table = spectra(voltages, coefficients)
    arrived = lax.ppermute(carried, "tm", [(i, i + 1) for i in range(n_time - 1)])
    current = spectra(voltages, coefficients, table)
    outgoing = messages(current, arrived, voltages.shape[0])
    received = lax.all_to_all(outgoing, ("tm", "inp"), split_axis=0, concat_axis=0, tiled=True)
    return visibilities(received, n_time, n_input)


def solution(mesh):
    in_specs = (P("inp", "tm"), P())
    out_specs = P(None, ("tm", "inp"), None, None)
    return jax.shard_map(shards, mesh=mesh, in_specs=in_specs, out_specs=out_specs, check_vma=False)
```

```python
import functools

import jax
import jax.numpy as jnp
import numpy as np
from jax import lax
from jax.experimental import pallas as pl
from jax.experimental.pallas import tpu as pltpu
from jax.sharding import PartitionSpec as P

NFFT = 8192
TAPS = 16
CH = 128
CH0 = 1024
LANES = 128
CHUNK = 512
HALF = NFFT // 2
GROUP = 8
FINE = 16
TILE = 512
SPAN = 8
BATCH = 1
DEPTH = 2
F32 = jnp.float32
BF16 = jnp.bfloat16


def turns(samples):
    channel = (CH0 + np.arange(CH)).reshape(CH // 2, 2).T
    angle = 2.0 * np.pi / NFFT * (samples[:, None, None] * channel % NFFT)
    return np.cos(angle), -np.sin(angle)


def twiddles():
    real, imag = (part.transpose(1, 0, 2) * NFFT ** (-0.5) for part in turns(np.arange(FINE)))
    fine = np.stack([np.concatenate([real, imag], axis=-1), np.concatenate([-imag, real], axis=-1)])
    coarse, base = (
        np.stack([np.concatenate([part] * 2, axis=-1) for part in turns(samples)], axis=1)
        for samples in (np.arange(0, CHUNK, FINE), np.arange(0, HALF, CHUNK))
    )
    return jnp.asarray(np.concatenate([part.reshape(-1, CH) for part in (fine, coarse, base)]), F32)


def split(value):
    high = value.astype(BF16)
    return high, (value - high.astype(F32)).astype(BF16)


def toeplitz_tree(coefficients, depth):
    size = (len(coefficients) + 1) // 2
    if depth == 0 or size == 1:
        return coefficients
    half = size // 2
    upper, middle, lower = (coefficients[k : k + size - 1] for k in (0, half, size))
    above = [a - b for a, b in zip(upper, middle)]
    below = [a - b for a, b in zip(lower, middle)]
    return [toeplitz_tree(part, depth - 1) for part in (middle, above, below)]


def weighted(pairs):
    parts = [coefficient * sample for coefficient, sample in pairs]
    while len(parts) > 1:
        parts = [parts[k] + parts[k + 1] if k + 1 < len(parts) else parts[k] for k in range(0, len(parts), 2)]
    return parts[0]


def toeplitz(tree, samples):
    size = len(samples)
    if len(tree) == 2 * size - 1 and not isinstance(tree[0], list):
        return [weighted((tree[size - 1 + i - j], samples[j]) for j in range(size)) for i in range(size)]
    half = size // 2
    first, second = samples[:half], samples[half:]
    both = toeplitz(tree[0], [a + b for a, b in zip(first, second)])
    above = toeplitz(tree[1], second)
    below = toeplitz(tree[2], first)
    return [a + b for a, b in zip(both, above)] + [a + b for a, b in zip(both, below)]


def coefficient_tree(taps):
    half = TAPS // 2
    taps = list(taps)
    near = toeplitz_tree(taps[1:half], DEPTH - 1)
    far = toeplitz_tree(taps[half + 1 :], DEPTH - 1)
    return taps, near, toeplitz_tree(taps[1:], DEPTH), far


def added(first, second):
    return [a + b for a, b in zip(first, second)]


def lower(taps, near, x):
    quarter = TAPS // 4
    inner = toeplitz(near, x[:quarter])
    first, second = (
        [weighted((taps[s - j], part[j]) for j in range(s + 1)) for s in range(quarter)]
        for part in (x[:quarter], x[quarter:])
    )
    return first + added(inner, second)


def upper(taps, far, x):
    quarter = TAPS // 4
    inner = toeplitz(far, x[quarter:])
    first, second = (
        [weighted((taps[TAPS + s - j], part[j]) for j in range(s + 1, quarter)) for s in range(quarter - 1)]
        for part in (x[:quarter], x[quarter:])
    )
    return added(inner, first) + inner[quarter - 1 :] + second


def later_frames(tree, x):
    taps, near, middle, far = tree
    half = TAPS // 2
    inner = toeplitz(middle, x[half:])
    return added(inner, upper(taps, far, x[:half])) + inner[half - 1 :] + upper(taps, far, x[half:])


def these_frames(tree, x):
    taps, near, middle, far = tree
    half = TAPS // 2
    inner = toeplitz(middle, x[:half])
    return lower(taps, near, x[:half]) + added(inner, lower(taps, near, x[half:]))


def ahead_copies(tiles_ref, coefficients_ref, ahead_ref, taps_ref, sems):
    width = CHUNK // LANES
    return [
        pltpu.make_async_copy(tiles_ref.at[:, :, :, pl.ds(0, width)], ahead_ref.at[0], sems.at[0]),
        pltpu.make_async_copy(coefficients_ref, taps_ref, sems.at[1]),
    ]


def block_copy(tiles_ref, ahead_ref, sems, step):
    width = CHUNK // LANES
    source = tiles_ref.at[:, :, :, pl.ds(step * width, width)]
    slot = lax.rem(step, 2)
    return pltpu.make_async_copy(source, ahead_ref.at[slot], sems.at[slot])


def channelize(carried, frames, inputs, *refs):
    step = pl.program_id(0)
    steps = HALF // CHUNK
    groups = inputs // GROUP
    if carried:
        x_ref, h_first, h_second, twiddle_ref, tiles_ref, coefficients_ref = refs[:6]
        out_ref, table_ref, ahead_ref, taps_ref, small_ref, sems = refs[6:]
        turn = lambda start, part, parity: twiddle_ref[pl.ds(start + 2 * part + parity, 1), :]
        sample = lambda group, s, part, block: x_ref[group, s, part, block]
        tap = lambda t, part, block: (h_first, h_second)[part][t : t + 1, block * LANES : (block + 1) * LANES]
        copies = ahead_copies(tiles_ref, coefficients_ref, ahead_ref, taps_ref, sems)

        @pl.when(step == 0)
        def _():
            for copy in copies:
                copy.start()

        @pl.when(step == steps - 1)
        def _():
            for copy in copies:
                copy.wait()
    else:
        tiles_ref, h_ref, table_ref, _, out_ref, ahead_ref, sems = refs
        slot = lax.rem(step, 2)
        sample = lambda group, s, part, block: ahead_ref[slot, group, s, part, block]

        def tap(t, part, block):
            start = pl.multiple_of(part * HALF + step * CHUNK + block * LANES, LANES)
            return h_ref[t : t + 1, pl.ds(start, LANES)]

        @pl.when(step > 0)
        def _():
            block_copy(tiles_ref, ahead_ref, sems, step).wait()

        @pl.when(step + 1 < steps)
        def _():
            block_copy(tiles_ref, ahead_ref, sems, step + 1).start()

    @pl.when(step == 0)
    def _():
        out_ref[...] = jnp.zeros_like(out_ref)
        if not carried:
            return
        for parity in range(2):
            starts = [(2 * part + parity) * FINE for part in range(2)]
            real, imag = (twiddle_ref[start : start + FINE] for start in starts)
            for k in range(CHUNK // FINE):
                at = slice(k * FINE, (k + 1) * FINE)
                turn_real, turn_imag = (turn(4 * FINE + 4 * k, part, parity) for part in range(2))
                small_ref[0, parity, at] = real * turn_real + imag * turn_imag
                small_ref[1, parity, at] = imag * turn_real - real * turn_imag

    lines = []
    trees = []
    for block in range(CHUNK // LANES):
        trees.append([])
        for part in range(2):
            taps = [jnp.broadcast_to(tap(t, part, block), (GROUP, LANES)) for t in range(TAPS)]
            trees[-1].append(coefficient_tree(taps))
    width = TILE // LANES
    for tile in range(CHUNK // TILE):
        lines.append([[], []])
        for start in range(0, groups, BATCH):
            batch = range(start, start + BATCH)
            columns = [[[], []] for _ in batch]
            for block in range(tile * width, (tile + 1) * width):
                first, second = (
                    [
                        (later_frames if carried else these_frames)(
                            trees[block][part], [sample(group, s, part, block).astype(F32) for s in range(frames)]
                        )
                        for group in batch
                    ]
                    for part in range(2)
                )
                for column, one, other in zip(columns, first, second):
                    for parity in range(2):
                        values = [a - b if parity else a + b for a, b in zip(one, other)]
                        if carried:
                            values.append(jnp.zeros((GROUP, LANES), F32))
                        pieces = [split(jnp.concatenate(values[s : s + 2], axis=0)) for s in range(0, frames, 2)]
                        column[parity].append([jnp.concatenate(part, axis=0) for part in zip(*pieces)])
            for column in columns:
                for parity in range(2):
                    lines[tile][parity].append([jnp.concatenate(part, axis=1) for part in zip(*column[parity])])

    rows = frames * GROUP
    here = pl.ds(pl.multiple_of(step * CHUNK, CHUNK), CHUNK)
    for parity in range(2):
        if carried:
            start = 4 * FINE + 4 * (CHUNK // FINE) + 4 * step
            wave = small_ref[0, parity] * turn(start, 0, parity) + small_ref[1, parity] * turn(start, 1, parity)
            table = jnp.concatenate(split(wave), axis=1)
            table_ref[parity, here] = table
        else:
            table = table_ref[parity, here]
        total = None
        for tile in range(CHUNK // TILE):
            line = lines[tile][parity]
            order = [line[first + k][part] for first in range(0, groups, SPAN) for part in range(2) for k in range(SPAN)]
            product = jnp.dot(
                jnp.concatenate(order, axis=0),
                table[tile * TILE : (tile + 1) * TILE],
                preferred_element_type=F32,
            )
            total = product if total is None else total + product
        for group in range(groups):
            place = 2 * (group // SPAN) * SPAN + group % SPAN
            both = total[place * rows : (place + 1) * rows] + total[(place + SPAN) * rows : (place + SPAN + 1) * rows]
            out_ref[parity, group * rows : (group + 1) * rows] += both[:, :CH] + both[:, CH:]


def assemble(frames, inputs, here_ref, before_ref, out_ref):
    groups = inputs // GROUP
    half = CH // 2
    for s in range(frames):
        sums = []
        for parity in range(2):
            spans = [slice((group * frames + s) * GROUP, (group * frames + s + 1) * GROUP) for group in range(groups)]
            sums.append(
                jnp.concatenate([here_ref[parity, span] + before_ref[parity, span] for span in spans], axis=0)
            )
        real = jnp.concatenate([part[:, :half] for part in sums], axis=1)
        imag = jnp.concatenate([part[:, half:] for part in sums], axis=1)
        turned = jnp.concatenate([real, imag], axis=0).T
        for parity in range(2):
            out_ref[:, parity, s, :] = turned[parity * half : (parity + 1) * half]


def messages(here, before, inputs):
    frames = here.shape[1] // inputs
    return pl.pallas_call(
        functools.partial(assemble, frames, inputs),
        out_shape=jax.ShapeDtypeStruct((CH // 2, 2, frames, 2 * inputs), F32),
        compiler_params=pltpu.CompilerParams(vmem_limit_bytes=16 * 2**20),
        name="messages",
    )(here, before).reshape(CH, frames, 2 * inputs)


def options(inputs, samples):
    rows = samples // NFFT * inputs
    return dict(
        grid=(HALF // CHUNK,),
        compiler_params=pltpu.CompilerParams(vmem_limit_bytes=40 * 2**20),
        cost_estimate=pl.CostEstimate(
            flops=4 * rows * NFFT * 2 * CH, bytes_accessed=2 * inputs * samples, transcendentals=0
        ),
    )


def spectra(voltages, coefficients):
    inputs, samples = voltages.shape
    frames = samples // NFFT
    steps = HALF // CHUNK
    whole, anywhere = pl.BlockSpec(memory_space=pltpu.VMEM), pl.BlockSpec(memory_space=pl.ANY)
    coefficients = pltpu.with_memory_space_constraint(coefficients, pltpu.HBM)
    waves = pltpu.with_memory_space_constraint(twiddles(), pltpu.HBM)
    tiles = voltages.reshape(inputs // GROUP, GROUP, samples // LANES, LANES).transpose(0, 2, 1, 3)
    tiles = tiles.reshape(inputs // GROUP, frames, 2, HALF // LANES, GROUP, LANES)
    block = (inputs // GROUP, frames, 2, CHUNK // LANES, GROUP, LANES)
    sums = jax.ShapeDtypeStruct((2, frames * inputs, CH), F32)
    ahead = jax.ShapeDtypeStruct((2,) + block, BF16)
    carried, table, ahead, taps = pl.pallas_call(
        functools.partial(channelize, True, frames, inputs),
        out_shape=(
            sums,
            jax.ShapeDtypeStruct((2, HALF, 2 * CH), BF16),
            ahead,
            jax.ShapeDtypeStruct(coefficients.shape, F32),
        ),
        in_specs=[
            pl.BlockSpec(block, lambda j: (0, 0, 0, j, 0, 0)),
            pl.BlockSpec((TAPS, CHUNK), lambda j: (0, j)),
            pl.BlockSpec((TAPS, CHUNK), lambda j: (0, steps + j)),
            pl.BlockSpec(waves.shape, lambda j: (0, 0)),
            anywhere,
            anywhere,
        ],
        out_specs=(whole,) * 4,
        scratch_shapes=[pltpu.VMEM((2, 2, CHUNK, CH), F32), pltpu.SemaphoreType.DMA((2,))],
        name="carried",
        **options(inputs, samples),
    )(tiles, coefficients, coefficients, waves, tiles, coefficients)

    def current():
        return pl.pallas_call(
            functools.partial(channelize, False, frames, inputs),
            out_shape=(sums, jax.ShapeDtypeStruct(ahead.shape, BF16)),
            in_specs=[anywhere, whole, whole, whole],
            out_specs=(whole, whole),
            scratch_shapes=[pltpu.SemaphoreType.DMA((2,))],
            input_output_aliases={3: 1},
            name="current",
            **options(inputs, samples),
        )(tiles, taps, table, ahead)[0]

    return carried, current


def correlate(n_time, n_input, inputs, frames, got_ref, out_ref, left_high, left_low, right_high, right_low):
    count = n_time * frames
    dot = functools.partial(jnp.dot, preferred_element_type=F32)

    @pl.when(pl.program_id(0) == 0)
    def _():
        for i in range(n_time):
            real_rows = slice(i * frames, (i + 1) * frames)
            imag_rows = slice(count + i * frames, count + (i + 1) * frames)
            for j in range(0, n_input, 2):
                lanes = slice(j * inputs, (j + 2) * inputs)
                first, second = got_ref[i * n_input + j], got_ref[i * n_input + j + 1]
                real = jnp.concatenate([first[:, :inputs], second[:, :inputs]], axis=1)
                imag = jnp.concatenate([first[:, inputs:], second[:, inputs:]], axis=1)
                real_high, real_low = split(real)
                imag_high, imag_low = split(imag)
                right_high[0, real_rows, lanes] = real_high
                right_low[0, real_rows, lanes] = real_low
                right_high[0, imag_rows, lanes] = imag_high
                right_low[0, imag_rows, lanes] = imag_low
                right_high[1, real_rows, lanes] = -imag_high
                right_low[1, real_rows, lanes] = -imag_low
                right_high[1, imag_rows, lanes] = real_high
                right_low[1, imag_rows, lanes] = real_low
        left_high[...] = right_high[0].T
        left_low[...] = right_low[0].T

    size = out_ref.shape[2]
    rows = pl.ds(pl.multiple_of(pl.program_id(0) * size, size), size)
    high, low = left_high[rows, :], left_low[rows, :]
    for part in range(2):
        total = dot(high, right_high[part]) + dot(high, right_low[part]) + dot(low, right_high[part])
        out_ref[part, 0] = total * (1.0 / count)


def visibilities(received, n_time, n_input):
    devices, frames, width = received.shape
    inputs = width // 2
    total = n_input * inputs
    depth = 2 * n_time * frames
    block = 256
    return pl.pallas_call(
        functools.partial(correlate, n_time, n_input, inputs, frames),
        out_shape=jax.ShapeDtypeStruct((2, 1, total, total), F32),
        grid=(total // block,),
        in_specs=[pl.BlockSpec(memory_space=pltpu.VMEM)],
        out_specs=pl.BlockSpec((2, 1, block, total), lambda j: (0, 0, j, 0)),
        scratch_shapes=[pltpu.VMEM((total, depth), BF16)] * 2 + [pltpu.VMEM((2, depth, total), BF16)] * 2,
        compiler_params=pltpu.CompilerParams(vmem_limit_bytes=48 * 2**20),
        name="correlate",
    )(received)


def shards(voltages, coefficients):
    n_time = lax.axis_size("tm")
    n_input = lax.axis_size("inp")
    carried, current = spectra(voltages, coefficients)
    arrived = lax.ppermute(carried, "tm", [(i, i + 1) for i in range(n_time - 1)])
    outgoing = messages(current(), arrived, voltages.shape[0])
    received = lax.all_to_all(outgoing, ("tm", "inp"), split_axis=0, concat_axis=0, tiled=True)
    return visibilities(received, n_time, n_input)


def solution(mesh):
    in_specs = (P("inp", "tm"), P())
    out_specs = P(None, ("tm", "inp"), None, None)
    return jax.shard_map(shards, mesh=mesh, in_specs=in_specs, out_specs=out_specs, check_vma=False)
```

```python
import functools

import jax
import jax.numpy as jnp
import numpy as np
from jax import lax
from jax.experimental import pallas as pl
from jax.experimental.pallas import tpu as pltpu
from jax.sharding import PartitionSpec as P

NFFT = 8192
TAPS = 16
CH = 128
CH0 = 1024
LANES = 128
CHUNK = 1024
HALF = NFFT // 2
GROUP = 8
FINE = 16
TILE = 1024
SPAN = 8
BATCH = 1
DEPTH = 2
F32 = jnp.float32
BF16 = jnp.bfloat16


def turns(samples):
    channel = (CH0 + np.arange(CH)).reshape(CH // 2, 2).T
    angle = 2.0 * np.pi / NFFT * (samples[:, None, None] * channel % NFFT)
    return np.cos(angle), -np.sin(angle)


def twiddles():
    real, imag = (part.transpose(1, 0, 2) * NFFT ** (-0.5) for part in turns(np.arange(FINE)))
    fine = np.stack([np.concatenate([real, imag], axis=-1), np.concatenate([-imag, real], axis=-1)])
    coarse, base = (
        np.stack([np.concatenate([part] * 2, axis=-1) for part in turns(samples)], axis=1)
        for samples in (np.arange(0, CHUNK, FINE), np.arange(0, HALF, CHUNK))
    )
    return jnp.asarray(np.concatenate([part.reshape(-1, CH) for part in (fine, coarse, base)]), F32)


def split(value):
    high = value.astype(BF16)
    return high, (value - high.astype(F32)).astype(BF16)


def toeplitz_tree(coefficients, depth):
    size = (len(coefficients) + 1) // 2
    if depth == 0 or size == 1:
        return coefficients
    half = size // 2
    upper, middle, lower = (coefficients[k : k + size - 1] for k in (0, half, size))
    above = [a - b for a, b in zip(upper, middle)]
    below = [a - b for a, b in zip(lower, middle)]
    return [toeplitz_tree(part, depth - 1) for part in (middle, above, below)]


def weighted(pairs):
    parts = [coefficient * sample for coefficient, sample in pairs]
    while len(parts) > 1:
        parts = [parts[k] + parts[k + 1] if k + 1 < len(parts) else parts[k] for k in range(0, len(parts), 2)]
    return parts[0]


def toeplitz(tree, samples):
    size = len(samples)
    if len(tree) == 2 * size - 1 and not isinstance(tree[0], list):
        return [weighted((tree[size - 1 + i - j], samples[j]) for j in range(size)) for i in range(size)]
    half = size // 2
    first, second = samples[:half], samples[half:]
    both = toeplitz(tree[0], [a + b for a, b in zip(first, second)])
    above = toeplitz(tree[1], second)
    below = toeplitz(tree[2], first)
    return [a + b for a, b in zip(both, above)] + [a + b for a, b in zip(both, below)]


def coefficient_tree(taps):
    half = TAPS // 2
    taps = list(taps)
    near = toeplitz_tree(taps[1:half], DEPTH - 1)
    far = toeplitz_tree(taps[half + 1 :], DEPTH - 1)
    return taps, near, toeplitz_tree(taps[1:], DEPTH), far


def added(first, second):
    return [a + b for a, b in zip(first, second)]


def lower(taps, near, x):
    quarter = TAPS // 4
    inner = toeplitz(near, x[:quarter])
    first, second = (
        [weighted((taps[s - j], part[j]) for j in range(s + 1)) for s in range(quarter)]
        for part in (x[:quarter], x[quarter:])
    )
    return first + added(inner, second)


def upper(taps, far, x):
    quarter = TAPS // 4
    inner = toeplitz(far, x[quarter:])
    first, second = (
        [weighted((taps[TAPS + s - j], part[j]) for j in range(s + 1, quarter)) for s in range(quarter - 1)]
        for part in (x[:quarter], x[quarter:])
    )
    return added(inner, first) + inner[quarter - 1 :] + second


def later_frames(tree, x):
    taps, near, middle, far = tree
    half = TAPS // 2
    inner = toeplitz(middle, x[half:])
    return added(inner, upper(taps, far, x[:half])) + inner[half - 1 :] + upper(taps, far, x[half:])


def these_frames(tree, x):
    taps, near, middle, far = tree
    half = TAPS // 2
    inner = toeplitz(middle, x[:half])
    return lower(taps, near, x[:half]) + added(inner, lower(taps, near, x[half:]))


def ahead_copies(tiles_ref, coefficients_ref, ahead_ref, taps_ref, sems):
    width = CHUNK // LANES
    return [
        pltpu.make_async_copy(tiles_ref.at[:, :, :, pl.ds(0, width)], ahead_ref.at[0], sems.at[0]),
        pltpu.make_async_copy(coefficients_ref, taps_ref, sems.at[1]),
    ]


def block_copy(tiles_ref, ahead_ref, sems, step):
    width = CHUNK // LANES
    source = tiles_ref.at[:, :, :, pl.ds(step * width, width)]
    slot = lax.rem(step, 2)
    return pltpu.make_async_copy(source, ahead_ref.at[slot], sems.at[slot])


def channelize(carried, frames, inputs, *refs):
    step = pl.program_id(0)
    steps = HALF // CHUNK
    groups = inputs // GROUP
    if carried:
        x_ref, h_first, h_second, twiddle_ref, tiles_ref, coefficients_ref = refs[:6]
        out_ref, table_ref, ahead_ref, taps_ref, small_ref, sems = refs[6:]
        turn = lambda start, part, parity: twiddle_ref[pl.ds(start + 2 * part + parity, 1), :]
        sample = lambda group, s, part, block: x_ref[group, s, part, block]
        tap = lambda t, part, block: (h_first, h_second)[part][t : t + 1, block * LANES : (block + 1) * LANES]
        copies = ahead_copies(tiles_ref, coefficients_ref, ahead_ref, taps_ref, sems)

        @pl.when(step == 0)
        def _():
            for copy in copies:
                copy.start()

        @pl.when(step == steps - 1)
        def _():
            for copy in copies:
                copy.wait()
    else:
        tiles_ref, h_ref, table_ref, _, out_ref, ahead_ref, sems = refs
        slot = lax.rem(step, 2)
        sample = lambda group, s, part, block: ahead_ref[slot, group, s, part, block]

        def tap(t, part, block):
            start = pl.multiple_of(part * HALF + step * CHUNK + block * LANES, LANES)
            return h_ref[t : t + 1, pl.ds(start, LANES)]

        @pl.when(step > 0)
        def _():
            block_copy(tiles_ref, ahead_ref, sems, step).wait()

        @pl.when(step + 1 < steps)
        def _():
            block_copy(tiles_ref, ahead_ref, sems, step + 1).start()

    @pl.when(step == 0)
    def _():
        out_ref[...] = jnp.zeros_like(out_ref)
        if not carried:
            return
        for parity in range(2):
            starts = [(2 * part + parity) * FINE for part in range(2)]
            real, imag = (twiddle_ref[start : start + FINE] for start in starts)
            for k in range(CHUNK // FINE):
                at = slice(k * FINE, (k + 1) * FINE)
                turn_real, turn_imag = (turn(4 * FINE + 4 * k, part, parity) for part in range(2))
                small_ref[0, parity, at] = real * turn_real + imag * turn_imag
                small_ref[1, parity, at] = imag * turn_real - real * turn_imag

    lines = []
    trees = []
    for block in range(CHUNK // LANES):
        trees.append([])
        for part in range(2):
            taps = [jnp.broadcast_to(tap(t, part, block), (GROUP, LANES)) for t in range(TAPS)]
            trees[-1].append(coefficient_tree(taps))
    width = TILE // LANES
    for tile in range(CHUNK // TILE):
        lines.append([[], []])
        for start in range(0, groups, BATCH):
            batch = range(start, start + BATCH)
            columns = [[[], []] for _ in batch]
            for block in range(tile * width, (tile + 1) * width):
                first, second = (
                    [
                        (later_frames if carried else these_frames)(
                            trees[block][part], [sample(group, s, part, block).astype(F32) for s in range(frames)]
                        )
                        for group in batch
                    ]
                    for part in range(2)
                )
                for column, one, other in zip(columns, first, second):
                    for parity in range(2):
                        values = [a - b if parity else a + b for a, b in zip(one, other)]
                        if carried:
                            values.append(jnp.zeros((GROUP, LANES), F32))
                        pieces = [split(jnp.concatenate(values[s : s + 2], axis=0)) for s in range(0, frames, 2)]
                        column[parity].append([jnp.concatenate(part, axis=0) for part in zip(*pieces)])
            for column in columns:
                for parity in range(2):
                    lines[tile][parity].append([jnp.concatenate(part, axis=1) for part in zip(*column[parity])])

    rows = frames * GROUP
    here = pl.ds(pl.multiple_of(step * CHUNK, CHUNK), CHUNK)
    for parity in range(2):
        if carried:
            start = 4 * FINE + 4 * (CHUNK // FINE) + 4 * step
            wave = small_ref[0, parity] * turn(start, 0, parity) + small_ref[1, parity] * turn(start, 1, parity)
            table = jnp.concatenate(split(wave), axis=1)
            table_ref[parity, here] = table
        else:
            table = table_ref[parity, here]
        total = None
        for tile in range(CHUNK // TILE):
            line = lines[tile][parity]
            order = [line[first + k][part] for first in range(0, groups, SPAN) for part in range(2) for k in range(SPAN)]
            product = jnp.dot(
                jnp.concatenate(order, axis=0),
                table[tile * TILE : (tile + 1) * TILE],
                preferred_element_type=F32,
            )
            total = product if total is None else total + product
        for group in range(groups):
            place = 2 * (group // SPAN) * SPAN + group % SPAN
            both = total[place * rows : (place + 1) * rows] + total[(place + SPAN) * rows : (place + SPAN + 1) * rows]
            out_ref[parity, group * rows : (group + 1) * rows] += both[:, :CH] + both[:, CH:]


def assemble(frames, inputs, here_ref, before_ref, out_ref):
    groups = inputs // GROUP
    half = CH // 2
    for s in range(frames):
        sums = []
        for parity in range(2):
            spans = [slice((group * frames + s) * GROUP, (group * frames + s + 1) * GROUP) for group in range(groups)]
            sums.append(
                jnp.concatenate([here_ref[parity, span] + before_ref[parity, span] for span in spans], axis=0)
            )
        real = jnp.concatenate([part[:, :half] for part in sums], axis=1)
        imag = jnp.concatenate([part[:, half:] for part in sums], axis=1)
        turned = jnp.concatenate([real, imag], axis=0).T
        for parity in range(2):
            out_ref[:, parity, s, :] = turned[parity * half : (parity + 1) * half]


def messages(here, before, inputs):
    frames = here.shape[1] // inputs
    return pl.pallas_call(
        functools.partial(assemble, frames, inputs),
        out_shape=jax.ShapeDtypeStruct((CH // 2, 2, frames, 2 * inputs), F32),
        compiler_params=pltpu.CompilerParams(vmem_limit_bytes=16 * 2**20),
        name="messages",
    )(here, before).reshape(CH, frames, 2 * inputs)


def options(inputs, samples):
    rows = samples // NFFT * inputs
    return dict(
        grid=(HALF // CHUNK,),
        compiler_params=pltpu.CompilerParams(vmem_limit_bytes=40 * 2**20),
        cost_estimate=pl.CostEstimate(
            flops=4 * rows * NFFT * 2 * CH, bytes_accessed=2 * inputs * samples, transcendentals=0
        ),
    )


def spectra(voltages, coefficients):
    inputs, samples = voltages.shape
    frames = samples // NFFT
    steps = HALF // CHUNK
    whole, anywhere = pl.BlockSpec(memory_space=pltpu.VMEM), pl.BlockSpec(memory_space=pl.ANY)
    coefficients = pltpu.with_memory_space_constraint(coefficients, pltpu.HBM)
    waves = pltpu.with_memory_space_constraint(twiddles(), pltpu.HBM)
    tiles = voltages.reshape(inputs // GROUP, GROUP, samples // LANES, LANES).transpose(0, 2, 1, 3)
    tiles = tiles.reshape(inputs // GROUP, frames, 2, HALF // LANES, GROUP, LANES)
    block = (inputs // GROUP, frames, 2, CHUNK // LANES, GROUP, LANES)
    sums = jax.ShapeDtypeStruct((2, frames * inputs, CH), F32)
    ahead = jax.ShapeDtypeStruct((2,) + block, BF16)
    carried, table, ahead, taps = pl.pallas_call(
        functools.partial(channelize, True, frames, inputs),
        out_shape=(
            sums,
            jax.ShapeDtypeStruct((2, HALF, 2 * CH), BF16),
            ahead,
            jax.ShapeDtypeStruct(coefficients.shape, F32),
        ),
        in_specs=[
            pl.BlockSpec(block, lambda j: (0, 0, 0, j, 0, 0)),
            pl.BlockSpec((TAPS, CHUNK), lambda j: (0, j)),
            pl.BlockSpec((TAPS, CHUNK), lambda j: (0, steps + j)),
            pl.BlockSpec(waves.shape, lambda j: (0, 0)),
            anywhere,
            anywhere,
        ],
        out_specs=(whole,) * 4,
        scratch_shapes=[pltpu.VMEM((2, 2, CHUNK, CH), F32), pltpu.SemaphoreType.DMA((2,))],
        name="carried",
        **options(inputs, samples),
    )(tiles, coefficients, coefficients, waves, tiles, coefficients)

    def current():
        return pl.pallas_call(
            functools.partial(channelize, False, frames, inputs),
            out_shape=(sums, jax.ShapeDtypeStruct(ahead.shape, BF16)),
            in_specs=[anywhere, whole, whole, whole],
            out_specs=(whole, whole),
            scratch_shapes=[pltpu.SemaphoreType.DMA((2,))],
            input_output_aliases={3: 1},
            name="current",
            **options(inputs, samples),
        )(tiles, taps, table, ahead)[0]

    return carried, current


def correlate(n_time, n_input, inputs, frames, got_ref, out_ref, left_high, left_low, right_high, right_low):
    count = n_time * frames
    dot = functools.partial(jnp.dot, preferred_element_type=F32)

    @pl.when(pl.program_id(0) == 0)
    def _():
        for i in range(n_time):
            real_rows = slice(i * frames, (i + 1) * frames)
            imag_rows = slice(count + i * frames, count + (i + 1) * frames)
            for j in range(0, n_input, 2):
                lanes = slice(j * inputs, (j + 2) * inputs)
                first, second = got_ref[i * n_input + j], got_ref[i * n_input + j + 1]
                real = jnp.concatenate([first[:, :inputs], second[:, :inputs]], axis=1)
                imag = jnp.concatenate([first[:, inputs:], second[:, inputs:]], axis=1)
                real_high, real_low = split(real)
                imag_high, imag_low = split(imag)
                right_high[0, real_rows, lanes] = real_high
                right_low[0, real_rows, lanes] = real_low
                right_high[0, imag_rows, lanes] = imag_high
                right_low[0, imag_rows, lanes] = imag_low
                right_high[1, real_rows, lanes] = -imag_high
                right_low[1, real_rows, lanes] = -imag_low
                right_high[1, imag_rows, lanes] = real_high
                right_low[1, imag_rows, lanes] = real_low
        left_high[...] = right_high[0].T
        left_low[...] = right_low[0].T

    size = out_ref.shape[2]
    rows = pl.ds(pl.multiple_of(pl.program_id(0) * size, size), size)
    high, low = left_high[rows, :], left_low[rows, :]
    for part in range(2):
        total = dot(high, right_high[part]) + dot(high, right_low[part]) + dot(low, right_high[part])
        out_ref[part, 0] = total * (1.0 / count)


def visibilities(received, n_time, n_input):
    devices, frames, width = received.shape
    inputs = width // 2
    total = n_input * inputs
    depth = 2 * n_time * frames
    block = 256
    return pl.pallas_call(
        functools.partial(correlate, n_time, n_input, inputs, frames),
        out_shape=jax.ShapeDtypeStruct((2, 1, total, total), F32),
        grid=(total // block,),
        in_specs=[pl.BlockSpec(memory_space=pltpu.VMEM)],
        out_specs=pl.BlockSpec((2, 1, block, total), lambda j: (0, 0, j, 0)),
        scratch_shapes=[pltpu.VMEM((total, depth), BF16)] * 2 + [pltpu.VMEM((2, depth, total), BF16)] * 2,
        compiler_params=pltpu.CompilerParams(vmem_limit_bytes=48 * 2**20),
        name="correlate",
    )(received)


def shards(voltages, coefficients):
    n_time = lax.axis_size("tm")
    n_input = lax.axis_size("inp")
    carried, current = spectra(voltages, coefficients)
    arrived = lax.ppermute(carried, "tm", [(i, i + 1) for i in range(n_time - 1)])
    outgoing = messages(current(), arrived, voltages.shape[0])
    received = lax.all_to_all(outgoing, ("tm", "inp"), split_axis=0, concat_axis=0, tiled=True)
    return visibilities(received, n_time, n_input)


def solution(mesh):
    in_specs = (P("inp", "tm"), P())
    out_specs = P(None, ("tm", "inp"), None, None)
    return jax.shard_map(shards, mesh=mesh, in_specs=in_specs, out_specs=out_specs, check_vma=False)
```

```python
import functools

import jax
import jax.numpy as jnp
import numpy as np
from jax import lax
from jax.experimental import pallas as pl
from jax.experimental.pallas import tpu as pltpu
from jax.sharding import PartitionSpec as P

NFFT = 8192
TAPS = 16
CH = 128
CH0 = 1024
LANES = 128
CHUNK = 1024
HALF = NFFT // 2
GROUP = 8
FINE = 16
TILE = 1024
SPAN = 8
BATCH = 1
DEPTH = 2
F32 = jnp.float32
BF16 = jnp.bfloat16


def turns(samples):
    channel = (CH0 + np.arange(CH)).reshape(CH // 2, 2).T
    angle = 2.0 * np.pi / NFFT * (samples[:, None, None] * channel % NFFT)
    return np.cos(angle), -np.sin(angle)


def twiddles():
    real, imag = (part.transpose(1, 0, 2) * NFFT ** (-0.5) for part in turns(np.arange(FINE)))
    fine = np.stack([np.concatenate([real, imag], axis=-1), np.concatenate([-imag, real], axis=-1)])
    coarse, base = (
        np.stack([np.concatenate([part] * 2, axis=-1) for part in turns(samples)], axis=1)
        for samples in (np.arange(0, CHUNK, FINE), np.arange(0, HALF, CHUNK))
    )
    return jnp.asarray(np.concatenate([part.reshape(-1, CH) for part in (fine, coarse, base)]), F32)


def split(value):
    high = value.astype(BF16)
    return high, (value - high.astype(F32)).astype(BF16)


def toeplitz_tree(coefficients, depth):
    size = (len(coefficients) + 1) // 2
    if depth == 0 or size == 1:
        return coefficients
    half = size // 2
    upper, middle, lower = (coefficients[k : k + size - 1] for k in (0, half, size))
    above = [a - b for a, b in zip(upper, middle)]
    below = [a - b for a, b in zip(lower, middle)]
    return [toeplitz_tree(part, depth - 1) for part in (middle, above, below)]


def weighted(pairs):
    parts = [coefficient * sample for coefficient, sample in pairs]
    while len(parts) > 1:
        parts = [parts[k] + parts[k + 1] if k + 1 < len(parts) else parts[k] for k in range(0, len(parts), 2)]
    return parts[0]


def toeplitz(tree, samples):
    size = len(samples)
    if len(tree) == 2 * size - 1 and not isinstance(tree[0], list):
        return [weighted((tree[size - 1 + i - j], samples[j]) for j in range(size)) for i in range(size)]
    half = size // 2
    first, second = samples[:half], samples[half:]
    both = toeplitz(tree[0], [a + b for a, b in zip(first, second)])
    above = toeplitz(tree[1], second)
    below = toeplitz(tree[2], first)
    return [a + b for a, b in zip(both, above)] + [a + b for a, b in zip(both, below)]


def coefficient_tree(taps):
    half = TAPS // 2
    taps = list(taps)
    near = toeplitz_tree(taps[1:half], DEPTH - 1)
    far = toeplitz_tree(taps[half + 1 :], DEPTH - 1)
    return taps, near, toeplitz_tree(taps[1:], DEPTH), far


def added(first, second):
    return [a + b for a, b in zip(first, second)]


def lower(taps, near, x):
    quarter = TAPS // 4
    inner = toeplitz(near, x[:quarter])
    first, second = (
        [weighted((taps[s - j], part[j]) for j in range(s + 1)) for s in range(quarter)]
        for part in (x[:quarter], x[quarter:])
    )
    return first + added(inner, second)


def upper(taps, far, x):
    quarter = TAPS // 4
    inner = toeplitz(far, x[quarter:])
    first, second = (
        [weighted((taps[TAPS + s - j], part[j]) for j in range(s + 1, quarter)) for s in range(quarter - 1)]
        for part in (x[:quarter], x[quarter:])
    )
    return added(inner, first) + inner[quarter - 1 :] + second


def later_frames(tree, x):
    taps, near, middle, far = tree
    half = TAPS // 2
    inner = toeplitz(middle, x[half:])
    return added(inner, upper(taps, far, x[:half])) + inner[half - 1 :] + upper(taps, far, x[half:])


def these_frames(tree, x):
    taps, near, middle, far = tree
    half = TAPS // 2
    inner = toeplitz(middle, x[:half])
    return lower(taps, near, x[:half]) + added(inner, lower(taps, near, x[half:]))


def ahead_copies(tiles_ref, coefficients_ref, ahead_ref, taps_ref, sems):
    width = CHUNK // LANES
    return [
        pltpu.make_async_copy(tiles_ref.at[:, :, :, pl.ds(0, width)], ahead_ref.at[0], sems.at[0]),
        pltpu.make_async_copy(coefficients_ref, taps_ref, sems.at[1]),
    ]


def block_copy(tiles_ref, ahead_ref, sems, step):
    width = CHUNK // LANES
    source = tiles_ref.at[:, :, :, pl.ds(step * width, width)]
    slot = lax.rem(step, 2)
    return pltpu.make_async_copy(source, ahead_ref.at[slot], sems.at[slot])


def channelize(carried, frames, inputs, *refs):
    step = pl.program_id(0)
    steps = HALF // CHUNK
    groups = inputs // GROUP
    if carried:
        x_ref, h_first, h_second, twiddle_ref, tiles_ref, coefficients_ref = refs[:6]
        out_ref, table_ref, ahead_ref, taps_ref, small_ref, sems = refs[6:]
        turn = lambda start, part, parity: twiddle_ref[pl.ds(start + 2 * part + parity, 1), :]
        sample = lambda group, s, part, block: x_ref[group, s, part, block]
        tap = lambda t, part, block: (h_first, h_second)[part][t : t + 1, block * LANES : (block + 1) * LANES]
        copies = ahead_copies(tiles_ref, coefficients_ref, ahead_ref, taps_ref, sems)

        @pl.when(step == 0)
        def _():
            for copy in copies:
                copy.start()

        @pl.when(step == steps - 1)
        def _():
            for copy in copies:
                copy.wait()
    else:
        tiles_ref, h_ref, table_ref, _, out_ref, ahead_ref, sems = refs
        slot = lax.rem(step, 2)
        sample = lambda group, s, part, block: ahead_ref[slot, group, s, part, block]

        def tap(t, part, block):
            start = pl.multiple_of(part * HALF + step * CHUNK + block * LANES, LANES)
            return h_ref[t : t + 1, pl.ds(start, LANES)]

        @pl.when(step > 0)
        def _():
            block_copy(tiles_ref, ahead_ref, sems, step).wait()

        @pl.when(step + 1 < steps)
        def _():
            block_copy(tiles_ref, ahead_ref, sems, step + 1).start()

    @pl.when(step == 0)
    def _():
        out_ref[...] = jnp.zeros_like(out_ref)
        if not carried:
            return
        for parity in range(2):
            starts = [(2 * part + parity) * FINE for part in range(2)]
            real, imag = (twiddle_ref[start : start + FINE] for start in starts)
            for k in range(CHUNK // FINE):
                at = slice(k * FINE, (k + 1) * FINE)
                turn_real, turn_imag = (turn(4 * FINE + 4 * k, part, parity) for part in range(2))
                small_ref[0, parity, at] = real * turn_real + imag * turn_imag
                small_ref[1, parity, at] = imag * turn_real - real * turn_imag

    lines = []
    trees = []
    for block in range(CHUNK // LANES):
        trees.append([])
        for part in range(2):
            taps = [jnp.broadcast_to(tap(t, part, block), (GROUP, LANES)) for t in range(TAPS)]
            trees[-1].append(coefficient_tree(taps))
    width = TILE // LANES
    for tile in range(CHUNK // TILE):
        lines.append([[], []])
        for start in range(0, groups, BATCH):
            batch = range(start, start + BATCH)
            columns = [[[], []] for _ in batch]
            for block in range(tile * width, (tile + 1) * width):
                first, second = (
                    [
                        (later_frames if carried else these_frames)(
                            trees[block][part], [sample(group, s, part, block).astype(F32) for s in range(frames)]
                        )
                        for group in batch
                    ]
                    for part in range(2)
                )
                for column, one, other in zip(columns, first, second):
                    for parity in range(2):
                        values = [a - b if parity else a + b for a, b in zip(one, other)]
                        if carried:
                            values.append(jnp.zeros((GROUP, LANES), F32))
                        pieces = [split(jnp.concatenate(values[s : s + 2], axis=0)) for s in range(0, frames, 2)]
                        column[parity].append([jnp.concatenate(part, axis=0) for part in zip(*pieces)])
            for column in columns:
                for parity in range(2):
                    lines[tile][parity].append([jnp.concatenate(part, axis=1) for part in zip(*column[parity])])

    rows = frames * GROUP
    here = pl.ds(pl.multiple_of(step * CHUNK, CHUNK), CHUNK)
    for parity in range(2):
        if carried:
            start = 4 * FINE + 4 * (CHUNK // FINE) + 4 * step
            wave = small_ref[0, parity] * turn(start, 0, parity) + small_ref[1, parity] * turn(start, 1, parity)
            table = jnp.concatenate(split(wave), axis=1)
            table_ref[parity, here] = table
        else:
            table = table_ref[parity, here]
        total = None
        for tile in range(CHUNK // TILE):
            line = lines[tile][parity]
            order = [line[first + k][part] for first in range(0, groups, SPAN) for part in range(2) for k in range(SPAN)]
            product = jnp.dot(
                jnp.concatenate(order, axis=0),
                table[tile * TILE : (tile + 1) * TILE],
                preferred_element_type=F32,
            )
            total = product if total is None else total + product
        for group in range(groups):
            place = 2 * (group // SPAN) * SPAN + group % SPAN
            both = total[place * rows : (place + 1) * rows] + total[(place + SPAN) * rows : (place + SPAN + 1) * rows]
            out_ref[parity, group * rows : (group + 1) * rows] += both[:, :CH] + both[:, CH:]


def assemble(frames, inputs, here_ref, before_ref, out_ref):
    groups = inputs // GROUP
    half = CH // 2
    for s in range(frames):
        sums = []
        for parity in range(2):
            spans = [slice((group * frames + s) * GROUP, (group * frames + s + 1) * GROUP) for group in range(groups)]
            sums.append(
                jnp.concatenate([here_ref[parity, span] + before_ref[parity, span] for span in spans], axis=0)
            )
        real = jnp.concatenate([part[:, :half] for part in sums], axis=1)
        imag = jnp.concatenate([part[:, half:] for part in sums], axis=1)
        turned = jnp.concatenate([real, imag], axis=0).T
        for parity in range(2):
            out_ref[:, parity, s, :] = turned[parity * half : (parity + 1) * half]


def messages(here, before, inputs):
    frames = here.shape[1] // inputs
    return pl.pallas_call(
        functools.partial(assemble, frames, inputs),
        out_shape=jax.ShapeDtypeStruct((CH // 2, 2, frames, 2 * inputs), F32),
        compiler_params=pltpu.CompilerParams(vmem_limit_bytes=16 * 2**20),
        name="messages",
    )(here, before).reshape(CH, frames, 2 * inputs)


def options(inputs, samples):
    rows = samples // NFFT * inputs
    return dict(
        grid=(HALF // CHUNK,),
        compiler_params=pltpu.CompilerParams(vmem_limit_bytes=40 * 2**20),
        cost_estimate=pl.CostEstimate(
            flops=4 * rows * NFFT * 2 * CH, bytes_accessed=2 * inputs * samples, transcendentals=0
        ),
    )


def spectra(voltages, coefficients):
    inputs, samples = voltages.shape
    frames = samples // NFFT
    steps = HALF // CHUNK
    whole, anywhere = pl.BlockSpec(memory_space=pltpu.VMEM), pl.BlockSpec(memory_space=pl.ANY)
    coefficients = pltpu.with_memory_space_constraint(coefficients, pltpu.HBM)
    waves = pltpu.with_memory_space_constraint(twiddles(), pltpu.HBM)
    tiles = voltages.reshape(inputs // GROUP, GROUP, samples // LANES, LANES).transpose(0, 2, 1, 3)
    tiles = tiles.reshape(inputs // GROUP, frames, 2, HALF // LANES, GROUP, LANES)
    block = (inputs // GROUP, frames, 2, CHUNK // LANES, GROUP, LANES)
    sums = jax.ShapeDtypeStruct((2, frames * inputs, CH), F32)
    ahead = jax.ShapeDtypeStruct((2,) + block, BF16)
    carried, table, ahead, taps = pl.pallas_call(
        functools.partial(channelize, True, frames, inputs),
        out_shape=(
            sums,
            jax.ShapeDtypeStruct((2, HALF, 2 * CH), BF16),
            ahead,
            jax.ShapeDtypeStruct(coefficients.shape, F32),
        ),
        in_specs=[
            pl.BlockSpec(block, lambda j: (0, 0, 0, j, 0, 0)),
            pl.BlockSpec((TAPS, CHUNK), lambda j: (0, j)),
            pl.BlockSpec((TAPS, CHUNK), lambda j: (0, steps + j)),
            pl.BlockSpec(waves.shape, lambda j: (0, 0)),
            anywhere,
            anywhere,
        ],
        out_specs=(whole,) * 4,
        scratch_shapes=[pltpu.VMEM((2, 2, CHUNK, CH), F32), pltpu.SemaphoreType.DMA((2,))],
        name="carried",
        **options(inputs, samples),
    )(tiles, coefficients, coefficients, waves, tiles, coefficients)

    def current():
        return pl.pallas_call(
            functools.partial(channelize, False, frames, inputs),
            out_shape=(sums, jax.ShapeDtypeStruct(ahead.shape, BF16)),
            in_specs=[anywhere, whole, whole, whole],
            out_specs=(whole, whole),
            scratch_shapes=[pltpu.SemaphoreType.DMA((2,))],
            input_output_aliases={3: 1},
            name="current",
            **options(inputs, samples),
        )(tiles, taps, table, ahead)[0]

    return carried, current


def correlate(n_time, n_input, inputs, frames, got_ref, out_ref, left_high, left_low, right_high, right_low):
    count = n_time * frames
    dot = functools.partial(jnp.dot, preferred_element_type=F32)

    part = pl.program_id(1)

    @pl.when((pl.program_id(0) == 0) & (part == 0))
    def _():
        for i in range(n_time):
            real_rows = slice(i * frames, (i + 1) * frames)
            imag_rows = slice(count + i * frames, count + (i + 1) * frames)
            for j in range(0, n_input, 2):
                lanes = slice(j * inputs, (j + 2) * inputs)
                first, second = got_ref[i * n_input + j], got_ref[i * n_input + j + 1]
                real = jnp.concatenate([first[:, :inputs], second[:, :inputs]], axis=1)
                imag = jnp.concatenate([first[:, inputs:], second[:, inputs:]], axis=1)
                real_high, real_low = split(real)
                imag_high, imag_low = split(imag)
                right_high[0, real_rows, lanes] = real_high
                right_low[0, real_rows, lanes] = real_low
                right_high[0, imag_rows, lanes] = imag_high
                right_low[0, imag_rows, lanes] = imag_low
                right_high[1, real_rows, lanes] = -imag_high
                right_low[1, real_rows, lanes] = -imag_low
                right_high[1, imag_rows, lanes] = real_high
                right_low[1, imag_rows, lanes] = real_low
        left_high[...] = right_high[0].T
        left_low[...] = right_low[0].T

    size = out_ref.shape[2]
    rows = pl.ds(pl.multiple_of(pl.program_id(0) * size, size), size)
    high, low = left_high[rows, :], left_low[rows, :]
    total = dot(high, right_high[part]) + dot(high, right_low[part]) + dot(low, right_high[part])
    out_ref[0, 0] = total * (1.0 / count)


def visibilities(received, n_time, n_input):
    devices, frames, width = received.shape
    inputs = width // 2
    total = n_input * inputs
    depth = 2 * n_time * frames
    block = 256
    return pl.pallas_call(
        functools.partial(correlate, n_time, n_input, inputs, frames),
        out_shape=jax.ShapeDtypeStruct((2, 1, total, total), F32),
        grid=(total // block, 2),
        in_specs=[pl.BlockSpec(memory_space=pltpu.VMEM)],
        out_specs=pl.BlockSpec((1, 1, block, total), lambda j, part: (part, 0, j, 0)),
        scratch_shapes=[pltpu.VMEM((total, depth), BF16)] * 2 + [pltpu.VMEM((2, depth, total), BF16)] * 2,
        compiler_params=pltpu.CompilerParams(vmem_limit_bytes=48 * 2**20),
        name="correlate",
    )(received)


def shards(voltages, coefficients):
    n_time = lax.axis_size("tm")
    n_input = lax.axis_size("inp")
    carried, current = spectra(voltages, coefficients)
    arrived = lax.ppermute(carried, "tm", [(i, i + 1) for i in range(n_time - 1)])
    outgoing = messages(current(), arrived, voltages.shape[0])
    received = lax.all_to_all(outgoing, ("tm", "inp"), split_axis=0, concat_axis=0, tiled=True)
    return visibilities(received, n_time, n_input)


def solution(mesh):
    in_specs = (P("inp", "tm"), P())
    out_specs = P(None, ("tm", "inp"), None, None)
    return jax.shard_map(shards, mesh=mesh, in_specs=in_specs, out_specs=out_specs, check_vma=False)
```
